128 devices in a mesh: dp: 32 (over z_hi, y, x), fsdp: 4 (over z_lo, core).
Axes of the slice: x: 4, y: 4, z: 4 (z_hi: 2, z_lo: 2; z = z_hi * 2 + z_lo), core: 2. Of those that a mesh axis runs over, the one named last changes fastest.
Arguments:
- tokens: bfloat16 [16384, 4096], P('dp'), may hold values from -6 to 6
- counts: int32 [32], P('dp'), may hold values from 256 to 512, as said below
- patch_index: int32 [16384], P('dp'), may hold values from 0 to 255
- clip_limit: float32 [], replicated, may hold values from 1024 to 8192
- norm_gain: float32 [4, 4096], replicated, may hold values from 0.25 to 1.75
- params: float32 [4, 4096, 4096], P(None, 'dp', 'fsdp'), may hold values from -0.09375 to 0.09375
- moments: float32 [4, 4096, 4096], P(None, 'dp', 'fsdp'), may hold values from -0.3 to 0.3
- seconds: float32 [4, 4096, 4096], P(None, 'dp', 'fsdp'), may hold values from 0.05 to 1
- gradients: float32 [4, 4096, 4096], P(None, 'dp', 'fsdp'), may hold values from -48 to 48
Outputs:
- params_new: float32 [4, 4096, 4096], P(None, 'dp', 'fsdp')
- moments_new: float32 [4, 4096, 4096], P(None, 'dp', 'fsdp')
- seconds_new: float32 [4, 4096, 4096], P(None, 'dp', 'fsdp')
- mixed: bfloat16 [16384, 4096], P('dp', 'fsdp')
The draws below stay inside these ranges and needn't reach their ends.
Inputs may be any that keep to these rules, and one draw needn't show every extreme that they name: `counts`: at most 512, reached on some index of dp in every draw.
All inputs are finite; a program needn't handle non-finite values.
Results may differ from the reference program's by a relative error of at most 0.0095.
Values may be sent and summed in bfloat16 or wider, within the bound.
A program may use at most 192 MiB of HBM per device.

```python
import math
import jax
import jax.numpy as jnp
from jax import lax

D = 4096
TOK_DEV = 512
LAYERS = 4
GRID = 16
STEP = 40
TOKENS = 16384
N_DP = 32


def draw_counts(key, part):
    drawn = jax.random.randint(key, (N_DP,), TOK_DEV // 2, TOK_DEV + 1)
    chosen = jax.random.randint(jax.random.fold_in(key, 3), (), 0, N_DP)
    return jnp.where(jnp.arange(N_DP) == chosen, TOK_DEV, drawn).astype(jnp.int32)


def draw_gradients(key, part):
    rising = jnp.arange(D, dtype=jnp.float32)[None, :, None] / D
    scaling = 1.0 + 2.0 * rising
    noise = jnp.clip(jax.random.normal(key, (LAYERS, D, D), jnp.float32), -6.0, 6.0)
    return scaling * noise


def with_ends(values, key, low, high):
    longest = values.shape.index(max(values.shape))
    spots = []
    for shift in (0, 1):
        where = [jax.random.randint(jax.random.fold_in(key, axis), (), 0, length) for axis, length in enumerate(values.shape)]
        where[longest] = (where[longest] + shift) % values.shape[longest]
        spots.append(tuple(where))
    return values.at[spots[0]].set(low).at[spots[1]].set(high)


def block_scale(own_key, shape, cuts, smallest, high):
    factor_of = 1.0
    for dim, shards_of in cuts:
        draws = jax.random.uniform(jax.random.fold_in(jax.random.fold_in(own_key, 6), dim), (shards_of,), jnp.float32, smallest / len(cuts), high / len(cuts))
        factor_of = factor_of * jnp.repeat(jnp.exp(draws), shape[dim] // shards_of).reshape((-1,) + (1,) * (len(shape) - 1 - dim))
    return factor_of


def normal_values(key, dims, deviation, limit, split=(), held_as=jnp.bfloat16):
    entries = jax.random.normal(key, dims, jnp.float32) * deviation
    if len(split) > 0:
        entries = block_scale(key, dims, split, -0.22, 0.18) * entries
    return jnp.clip(entries, min=-limit, max=limit).astype(held_as)


def setup_inputs(seed: int = 0) -> dict:
    seeds = jax.random.split(jax.random.key(seed), 10)
    tokens = normal_values(seeds[0], (TOKENS, D), 1.0, 6.0, ((0, 32),))
    counts = draw_counts(jax.random.fold_in(seeds[9], 71), 0)
    patch_index = with_ends(jax.random.randint(seeds[2], (TOKENS,), 0, GRID * GRID), jax.random.fold_in(seeds[2], 1), 0, (GRID * GRID) - 1).astype(jnp.int32)
    clip_limit = jnp.clip(jnp.exp(jax.random.uniform(seeds[3], (), jnp.float32, math.log(1024.0), math.log(8192.0))), 1024.0, 8192.0)
    norm_gain = jnp.clip(1.0 + 0.15 * jax.random.normal(seeds[4], (LAYERS, D), jnp.float32), 0.25, 1.75)
    params = normal_values(seeds[5], (LAYERS, D, D), D ** -0.5, 0.09375, ((1, 32), (2, 4)), jnp.float32)
    moments = normal_values(seeds[6], (LAYERS, D, D), 0.05, 0.3, ((1, 32), (2, 4)), jnp.float32)
    seconds = jnp.clip(jnp.exp(math.log(1.0) - 2.9957323 * jax.random.uniform(seeds[7], (LAYERS, D, D), jnp.float32) ** block_scale(seeds[7], (LAYERS, D, D), ((1, 32), (2, 4)), -0.2, 0.2)), 0.05, 1.0)
    gradients = draw_gradients(jax.random.fold_in(seeds[9], 71), 0)
    return dict(tokens=tokens, counts=counts, patch_index=patch_index, clip_limit=clip_limit, norm_gain=norm_gain, params=params, moments=moments, seconds=seconds, gradients=gradients)


beta_one = 0.9
beta_two = 0.95
adam_eps = 1e-08
learning_rate = 0.0024
weight_decay = 0.05
norm_eps = 1e-06

def position_code(patch_index):
    quarter = D // 4
    freqs = 1.0 / 10000.0 ** (jnp.arange(quarter, dtype=jnp.float32) / quarter)
    across = (patch_index // GRID).astype(jnp.float32)[:, None] * freqs[None, :]
    downward = (patch_index % GRID).astype(jnp.float32)[:, None] * freqs[None, :]
    return jnp.concatenate([jnp.sin(across), jnp.cos(across), jnp.sin(downward), jnp.cos(downward)], axis=1)

def layer_norm(stream, gain_row):
    centre = lax.optimization_barrier(jnp.mean(stream, axis=1, keepdims=True))
    shifted = stream - centre
    spread = lax.optimization_barrier(jnp.mean(shifted * shifted, axis=1, keepdims=True))
    return (shifted * lax.rsqrt(spread + norm_eps) * gain_row[None, :]).astype(jnp.bfloat16)

def adam_update(params, moments, seconds, gradients, factor):
    clipped = gradients * factor
    moments_new = beta_one * moments + (1.0 - beta_one) * clipped
    seconds_new = beta_two * seconds + (1.0 - beta_two) * clipped * clipped
    direction = moments_new / (1.0 - beta_one ** STEP) / (jnp.sqrt(seconds_new / (1.0 - beta_two ** STEP)) + adam_eps)
    params_new = params - learning_rate * (direction + weight_decay * params)
    return (params_new, moments_new, seconds_new)

def reference(tokens, counts, patch_index, clip_limit, norm_gain, params, moments, seconds, gradients):
    squares = jnp.sum(gradients * gradients)
    factor = jnp.minimum(1.0, clip_limit / (jnp.sqrt(squares) + 1e-06))
    params_new, moments_new, seconds_new = adam_update(params, moments, seconds, gradients, factor)
    weights = params_new.astype(jnp.bfloat16)
    slot = jnp.arange(TOKENS, dtype=jnp.int32) % TOK_DEV
    valid = (slot < jnp.repeat(counts, TOK_DEV, total_repeat_length=TOKENS))[:, None]
    stream = jnp.where(valid, tokens.astype(jnp.float32) + position_code(patch_index), 0.0)
    for current in range(LAYERS):
        normed = layer_norm(stream, norm_gain[current])
        branch = jnp.dot(normed, weights[current], preferred_element_type=jnp.float32).astype(jnp.bfloat16)
        stream = stream + branch.astype(jnp.float32)
    mixed = jnp.where(valid, stream, 0.0).astype(jnp.bfloat16)
    return (params_new, moments_new, seconds_new, mixed)
```

```python
import functools
import math

import jax
import jax.numpy as jnp
from jax import lax
from jax.experimental import pallas as pl
from jax.experimental.pallas import tpu as pltpu
from jax.sharding import PartitionSpec as P

D = 4096
LAYERS = 4
STEP = 40
ROWS = 128
HALF = 512
CHUNKS = 4
STEPS = LAYERS * CHUNKS

beta_one = 0.9
beta_two = 0.95
adam_eps = 1e-08
learning_rate = 0.0024
weight_decay = 0.05
norm_eps = 1e-06
BF = jnp.bfloat16
F32 = jnp.float32
MESH = pl.DeviceIdType.MESH


def kernel(
    tokens_hbm, counts_ref, patch_ref, clip_ref, gain_ref, params_hbm, moments_hbm, seconds_hbm,
    gradients_hbm, params_out, moments_out, seconds_out, mixed_out,
    pv, mv, vv, gv, wsh, wb, tok, oth, xbuf, stream, ysend, yrecv, acc, full, statbuf, msend,
    table, valid, meta_s, meta_r, red,
    in_sem, out_sem, tok_sem, red_s, red_r, wx_s, wx_r, ag_s, ag_r, ts_s, ts_r,
    y_s, y_r, xd_s, xd_r, xi_s, xi_r, f_s, f_r, st_s, st_r, fin_s, fin_r,
):
    dp = lax.axis_index("dp")
    fs = lax.axis_index("fsdp")
    x = dp % 4
    y = (dp // 4) % 4
    zh = dp // 16
    zl = fs // 2
    c = fs % 2
    b = zh
    a = (zl + zh) % 2
    mine = 2 * a + c

    def flip(v, bit):
        return 1 - v if bit else v

    def at(xx, yy, hh, ll, cc):
        return (hh * 16 + yy * 4 + xx, ll * 2 + cc)

    def along_x(d):
        return at((x + d) % 4, y, zh, zl, c)

    def along_y(d):
        return at(x, (y + d) % 4, zh, zl, c)

    def column(r):
        return at(x, y, flip(zh, r & 4), flip(zl, r & 2), flip(c, r & 1))

    def block_of(r):
        return 2 * flip(a, r & 2) + flip(c, r & 1)

    core_peer = column(1)
    x_peer = column(2)
    y_peer = column(6)

    def remote(src, dst, ssem, rsem, dev):
        return pltpu.make_async_remote_copy(
            src_ref=src, dst_ref=dst, send_sem=ssem, recv_sem=rsem, device_id=dev,
            device_id_type=MESH,
        )

    for l in range(LAYERS):
        pltpu.make_async_copy(gradients_hbm.at[l], gv.at[l], in_sem.at[l, 3]).start()
    barrier = pltpu.get_barrier_semaphore()
    others = [along_x(d) for d in (1, 2, 3)] + [along_y(d) for d in (1, 2, 3)]
    others += [column(r) for r in range(1, 8)]
    for dev in others:
        pl.semaphore_signal(barrier, inc=1, device_id=dev, device_id_type=MESH)
    for l in range(LAYERS):
        for j, (src, dst) in enumerate(((params_hbm, pv), (moments_hbm, mv), (seconds_hbm, vv))):
            pltpu.make_async_copy(src.at[l], dst.at[l], in_sem.at[l, j]).start()
    for q in range(4):
        pltpu.make_async_copy(
            tokens_hbm.at[:, pl.ds(1024 * q, 1024)], tok.at[q], tok_sem.at[q]
        ).start()

    total = jnp.zeros((8, 1024), F32)
    for l in range(LAYERS):
        pltpu.make_async_copy(gradients_hbm.at[l], gv.at[l], in_sem.at[l, 3]).wait()

        def squares(i, part, l=l):
            g = gv[l, pl.ds(pl.multiple_of(i * 32, 32), 32), :]
            g = g * g
            return part + (g[0:8] + g[8:16]) + (g[16:24] + g[24:32])

        total = lax.fori_loop(0, 4, squares, total)
    tile = total[:, 0:128]
    for i in range(1, 8):
        tile = tile + total[:, 128 * i : 128 * (i + 1)]
    pl.semaphore_wait(barrier, len(others))

    def exchange(stage, devs, tile, filler):
        red[stage, 0] = tile
        copies = [
            remote(
                red.at[stage, 0], red.at[stage, r + 1], red_s.at[stage, r], red_r.at[stage, r], dev
            )
            for r, dev in enumerate(devs)
        ]
        for copy in copies:
            copy.start()
        filler()
        for r, copy in enumerate(copies):
            copy.wait()
            tile = tile + red[stage, r + 1]
        return tile

    def token_copy():
        return remote(
            tok.at[2 * (1 - b) + c], oth.at[c], ts_s.at[0], ts_r.at[0], y_peer
        )

    def fill_column():
        for q in range(4):
            pltpu.make_async_copy(
                tokens_hbm.at[:, pl.ds(1024 * q, 1024)], tok.at[q], tok_sem.at[q]
            ).wait()
        token_copy().start()

    def fill_table():
        lane = lax.broadcasted_iota(jnp.int32, (16, 1024), 1).astype(F32)
        row = lax.broadcasted_iota(jnp.int32, (16, 1024), 0).astype(F32)
        angle = row * jnp.exp(lane * (-math.log(10000.0) / 1024.0))
        for q, wave in ((0, jnp.sin(angle)), (1, jnp.cos(angle))):
            cols = slice(1024 * q, 1024 * (q + 1))
            for i in range(3):
                piece = wave.astype(BF)
                table[16 * i : 16 * (i + 1), cols] = piece
                wave = wave - piece.astype(F32)
        table[48:128, :] = jnp.zeros((80, 2048), BF)

    tile = exchange(0, [column(r) for r in range(1, 8)], tile, fill_column)
    tile = exchange(1, [along_x(d) for d in (1, 2, 3)], tile, fill_table)
    tile = exchange(2, [along_y(d) for d in (1, 2, 3)], tile, lambda: None)
    norm = jnp.sqrt(jnp.sum(jnp.sum(tile, axis=1, keepdims=True), axis=0, keepdims=True))
    factor = jnp.minimum(1.0, clip_ref[0, 0] / (norm + 1e-06))

    def weight_copies(l):
        here = wb.at[l, zl, y, x]
        keep = pltpu.make_async_copy(wsh.at[l, c], here, wx_r.at[l, 0])
        give = remote(wsh.at[l, 1 - c], here, wx_s.at[l, 0], wx_r.at[l, 0], core_peer)
        same = remote(wsh.at[l, c], here, wx_s.at[l, 0], wx_r.at[l, 1], x_peer)
        cross = remote(wsh.at[l, 1 - c], here, wx_s.at[l, 1], wx_r.at[l, 1], column(3))
        return keep, give, same, cross

    for l in range(LAYERS):
        for j, (src, dst) in enumerate(((params_hbm, pv), (moments_hbm, mv), (seconds_hbm, vv))):
            pltpu.make_async_copy(src.at[l], dst.at[l], in_sem.at[l, j]).wait()

        def update(i, _, l=l):
            rows = pl.ds(pl.multiple_of(i * 16, 16), 16)
            p = pv[l, rows, :]
            clipped = gv[l, rows, :] * factor
            m = beta_one * mv[l, rows, :] + (1.0 - beta_one) * clipped
            v = beta_two * vv[l, rows, :] + (1.0 - beta_two) * clipped * clipped
            root = jnp.sqrt(v * (1.0 / (1.0 - beta_two**STEP))) + adam_eps
            direction = (m * (1.0 / (1.0 - beta_one**STEP))) / root
            p = p - learning_rate * (direction + weight_decay * p)
            mv[l, rows, :] = m
            vv[l, rows, :] = v
            pv[l, rows, :] = p
            w = p.astype(BF)
            wsh[l, 0, rows, :] = w[:, 0:HALF]
            wsh[l, 1, rows, :] = w[:, HALF:]
            return 0

        lax.fori_loop(0, ROWS // 16, update, 0)
        keep, give, same, cross = weight_copies(l)

        @pl.when(c == a)
        def _():
            keep.start()
            give.start()

        @pl.when(c != a)
        def _():
            same.start()
            cross.start()

    def start_outputs():
        for l in range(LAYERS):
            for j, (src, dst) in enumerate(((pv, params_out), (mv, moments_out), (vv, seconds_out))):
                pltpu.make_async_copy(src.at[l], dst.at[l], out_sem.at[l, j]).start()

    def piece(l, h, phase, xx, yy, part):
        if phase == 0:
            return wb.at[l, h, yy, xx, pl.ds(64 * part, 64), :]
        if h == 0:
            return wb.at[l, 0, yy, pl.ds(2 * part, 2)]
        return wb.at[l, 1, pl.ds(2 * part, 2), xx]

    def gather_copy(l, h, phase, sign, kind):
        on_x = (h == 0) == (phase == 0)
        step = 1 if sign == 0 else 3
        part = sign if kind != 1 else 1 - sign
        xx, yy = x, y
        if kind == 2:
            if on_x:
                xx = (x + 4 - step) % 4
            else:
                yy = (y + 4 - step) % 4
        ref = piece(l, h, phase, xx, yy, part)
        slot = ((h * 2 + phase) * 2 + sign) * 3 + kind
        dev = along_x(step) if on_x else along_y(step)
        return remote(ref, ref, ag_s.at[l, slot], ag_r.at[l, slot], dev)

    def both(l, phase, kind):
        return [gather_copy(l, h, phase, sign, kind) for h in (0, 1) for sign in (0, 1)]

    def start_all(copies):
        for copy in copies:
            copy.start()

    def recv_all(copies):
        for copy in copies:
            copy.wait_recv()

    def own_out(l):
        keep, give, same, cross = weight_copies(l)
        keep.wait()
        cross.wait_recv()
        start_all(both(l, 0, 0))
        start_all(both(l, 0, 1))

    def own_on(l):
        recv_all(both(l, 0, 0))
        start_all(both(l, 0, 2))

    def line_out(l):
        recv_all(both(l, 0, 1))
        recv_all(both(l, 0, 2))
        start_all(both(l, 1, 0))
        start_all(both(l, 1, 1))

    def line_on(l):
        recv_all(both(l, 1, 0))
        start_all(both(l, 1, 2))

    def plane_done(l):
        recv_all(both(l, 1, 1))
        recv_all(both(l, 1, 2))

    lane = lax.broadcasted_iota(jnp.int32, (ROWS, 128), 1)
    lane_f = lane.astype(F32)

    def spread(index):
        hit = (lane_f == index) | (lane_f == index + 16.0) | (lane_f == index + 32.0)
        return jnp.where(hit, 1.0, 0.0).astype(BF)

    def code(index, q):
        return jnp.dot(
            spread(index), table[:, 1024 * q : 1024 * (q + 1)], preferred_element_type=F32
        )

    def place(k, side, half, centre, scale):
        for q in range(2):
            for h in range(2):
                i = 2 * q + h
                values = half[q][:, HALF * h : HALF * (h + 1)]
                gain = gain_ref[pl.ds(4 * b + i, 1), :]
                xbuf[0, k, i, side] = ((values - centre) * scale * gain).astype(BF)

                @pl.when(mine == i)
                def _(values=values):
                    stream[k, side] = values

    def embed_own(k):
        rows = slice(ROWS * k, ROWS * (k + 1))
        p = patch_ref[rows, :]
        high = (p // 16).astype(F32)
        low = (p % 16).astype(F32)
        slot = lax.broadcasted_iota(jnp.int32, (ROWS, 1), 0) + ROWS * k
        real = jnp.where(slot < counts_ref[0, 0], 1.0, 0.0)
        centre = jnp.zeros((ROWS, 1), F32)
        for q in range(4):
            values = tok[q, rows, :].astype(F32) + code(high if q < 2 else low, q % 2)
            values = jnp.where(real > 0.5, values, 0.0)
            full[q] = values
            centre = centre + jnp.sum(values, axis=1, keepdims=True)
        centre = centre * (1.0 / D)
        square = jnp.zeros((ROWS, 1), F32)
        for q in range(4):
            shifted = full[q] - centre
            square = square + jnp.sum(shifted * shifted, axis=1, keepdims=True)
        scale = lax.rsqrt(square * (1.0 / D) + norm_eps)
        place(k, zh, [full[2 * b], full[2 * b + 1]], centre, scale)
        valid[k, zh] = real
        cols = jnp.zeros((ROWS, 128), F32)
        for i, value in enumerate((centre, scale, high, low, real)):
            cols = jnp.where(lane == i, value, cols)
        meta_s[k] = cols.T[0:8, :]

    def meta_copy():
        return remote(meta_s, meta_r, ts_s.at[1], ts_r.at[1], y_peer)

    def share_copy():
        return remote(oth.at[c], oth.at[c], ts_s.at[2], ts_r.at[2], core_peer)

    def embed_other(k):
        rows = slice(ROWS * k, ROWS * (k + 1))
        cols = jnp.concatenate([meta_r[k]] * 16, axis=0).T
        centre, scale, high, low, real = [cols[:, i : i + 1] for i in range(5)]
        index = jnp.where(b == 0, high, low)
        half = []
        for q in range(2):
            values = oth[q, rows, :].astype(F32) + code(index, q)
            half.append(jnp.where(real > 0.5, values, 0.0))
        place(k, 1 - zh, half, centre, scale)
        valid[k, 1 - zh] = real

    own_out(0)
    embed_own(0)
    own_on(0)
    embed_own(1)
    line_out(0)
    own_out(1)
    embed_own(2)
    embed_own(3)
    meta_copy().start()
    start_outputs()
    own_on(1)
    line_on(0)
    token_copy().wait_recv()
    share_copy().start()
    meta_copy().wait_recv()
    share_copy().wait_recv()
    for k in range(CHUNKS):
        embed_other(k)
    own_out(2)
    line_out(1)

    def y_copy(k):
        return remote(ysend.at[k], yrecv.at[k], y_s.at[k], y_r.at[k], y_peer)

    def core_copy(s):
        ref = xbuf.at[(s // 4 + 1) % 2, s % 4, mine]
        return remote(ref, ref, xd_s.at[s % 8], xd_r.at[s % 8], core_peer)

    def chip_copy(s):
        ref = xbuf.at[(s // 4 + 1) % 2, s % 4, mine]
        return remote(ref, ref, xi_s.at[s % 8], xi_r.at[s % 8], x_peer)

    def pass_copy(s):
        ref = xbuf.at[(s // 4 + 1) % 2, s % 4, block_of(2)]
        return remote(ref, ref, f_s.at[s % 8], f_r.at[s % 8], core_peer)

    def stat_copies(s):
        return [
            remote(
                statbuf.at[s, 0], statbuf.at[s, r], st_s.at[s % 8, r], st_r.at[s % 8, r], column(r)
            )
            for r in range(1, 8)
        ]

    def final_copies(k):
        dst = mixed_out.at[pl.ds(k * ROWS, ROWS), pl.ds(pl.multiple_of(c * HALF, HALF), HALF)]
        return [
            remote(
                msend.at[k, t], dst, fin_s.at[k, t], fin_r.at[k, c], at(x, y, t, b, a)
            )
            for t in (0, 1)
        ]

    def final_recv(k, part):
        dst = mixed_out.at[pl.ds(k * ROWS, ROWS), pl.ds(part * HALF, HALF)]
        return pltpu.make_async_copy(msend.at[k, 0], dst, fin_r.at[k, part])

    def normalise(s):
        last = s - 4
        l, k = s // 4, s % 4
        means = [statbuf[last, r, 0:1, :] for r in range(8)]
        mean = means[0]
        for r in range(1, 8):
            mean = mean + means[r]
        mean = mean * 0.125
        spread_sum = jnp.zeros_like(mean)
        for r in range(8):
            off = means[r] - mean
            spread_sum = spread_sum + (statbuf[last, r, 1:2, :] + float(HALF) * off * off)
        scale = lax.rsqrt(spread_sum * (1.0 / D) + norm_eps)
        rows = jnp.concatenate([means[r] - mean for r in range(4)] + [scale] * 4, axis=0)
        cols = jnp.concatenate([rows] * 16, axis=0).T
        scale = cols[:, 4:5]
        for r in range(4):
            i = block_of(r)
            off = cols[:, r : r + 1]
            gain = gain_ref[pl.ds(8 * l + 4 * b + i, 1), :]
            d = xbuf[l % 2, k, i].reshape(2 * ROWS, HALF).astype(F32)
            xbuf[l % 2, k, i] = ((d + off) * scale * gain).astype(BF).reshape(2, ROWS, HALF)

    def multiply(s):
        l, k = s // 4, s % 4
        left = jnp.concatenate(
            [xbuf[l % 2, k, i].reshape(2 * ROWS, HALF) for i in range(4)], axis=1
        )

        def column_tile(n, _):
            h = n // 2
            cols = pl.ds(pl.multiple_of((n % 2) * 256, 256), 256)
            right = wb[l, h, :, :, :, cols].reshape(2048, 256)
            acc[h, :, cols] = jnp.dot(left, right, preferred_element_type=F32)
            return 0

        lax.fori_loop(0, 4, column_tile, 0)
        ysend[k] = acc[1 - b].astype(BF).reshape(2, ROWS, HALF)
        stream[k] = stream[k] + acc[b].reshape(2, ROWS, HALF)
        y_copy(k).start()

    def receive(s):
        k = s % 4
        y_copy(k).wait_recv()
        values = (stream[k] + yrecv[k].astype(F32)).reshape(2 * ROWS, HALF)

        @pl.when(s < STEPS - 4)
        def _():
            stream[k] = values.reshape(2, ROWS, HALF)
            mean = jnp.sum(values, axis=1, keepdims=True) * (1.0 / HALF)
            d = values - mean
            square = jnp.sum(d * d, axis=1, keepdims=True)
            lanes = lax.broadcasted_iota(jnp.int32, (2 * ROWS, 128), 1)
            cols = jnp.where(lanes == 0, mean, jnp.where(lanes == 1, square, 0.0))
            statbuf[s, 0] = cols.T[0:8, :]
            xbuf[(s // 4 + 1) % 2, k, mine] = d.astype(BF).reshape(2, ROWS, HALF)
            start_all(stat_copies(s))
            chip_copy(s).start()
            core_copy(s).start()

        @pl.when(s >= STEPS - 4)
        def _():
            keep = jnp.concatenate([valid[k, 0], valid[k, 1]], axis=0) > 0.5
            msend[k] = jnp.where(keep, values, 0.0).astype(BF).reshape(2, ROWS, HALF)
            for t, copy in enumerate(final_copies(k)):
                here = (zh == t) & (zl == b) & (c == a)

                @pl.when(here)
                def _(t=t):
                    dst = mixed_out.at[
                        pl.ds(k * ROWS, ROWS), pl.ds(pl.multiple_of(c * HALF, HALF), HALF)
                    ]
                    pltpu.make_async_copy(msend.at[k, t], dst, fin_r.at[k, c]).start()

                @pl.when(jnp.logical_not(here))
                def _(copy=copy):
                    copy.start()

    def body(s, _):
        slot = s // 4 + 1

        @pl.when(s % 4 == 0)
        def _():
            @pl.when(s < STEPS)
            def _():
                plane_done(s // 4)

        @pl.when(s % 4 == 1)
        def _():
            @pl.when(slot + 1 < LAYERS)
            def _():
                own_on(slot + 1)

            @pl.when(slot < LAYERS)
            def _():
                line_on(slot)

        @pl.when(s % 4 == 2)
        def _():
            @pl.when(slot + 2 < LAYERS)
            def _():
                own_out(slot + 2)

            @pl.when(slot + 1 < LAYERS)
            def _():
                line_out(slot + 1)

        @pl.when((s >= 4) & (s < STEPS))
        def _():
            last = s - 4
            chip_copy(last).wait_recv()
            pass_copy(last).start()
            y_copy(s % 4).wait_send()
            for copy in stat_copies(last):
                copy.wait()
            core_copy(last).wait()
            chip_copy(last).wait_send()
            pass_copy(last).wait()
            normalise(s)

        @pl.when(s < STEPS)
        def _():
            multiply(s)

        @pl.when(s >= 2)
        def _():
            receive(s - 2)

        return 0

    lax.fori_loop(0, STEPS + 2, body, 0)

    for k in range(CHUNKS):
        for part in (0, 1):
            final_recv(k, part).wait()
        y_copy(k).wait_send()
        for t, copy in enumerate(final_copies(k)):
            here = (zh == t) & (zl == b) & (c == a)

            @pl.when(jnp.logical_not(here))
            def _(copy=copy):
                copy.wait_send()

    token_copy().wait_send()
    meta_copy().wait_send()
    share_copy().wait_send()
    for l in range(LAYERS):
        for phase in (0, 1):
            for kind in (0, 1, 2):
                for copy in both(l, phase, kind):
                    copy.wait_send()
        keep, give, same, cross = weight_copies(l)

        @pl.when(c == a)
        def _():
            give.wait_send()

        @pl.when(c != a)
        def _():
            same.wait_send()
            cross.wait_send()

        for j, (src, dst) in enumerate(((pv, params_out), (mv, moments_out), (vv, seconds_out))):
            pltpu.make_async_copy(src.at[l], dst.at[l], out_sem.at[l, j]).wait()


def per_device(
    tokens, counts, patch_index, clip_limit, norm_gain, params, moments, seconds, gradients
):
    any_space = pl.BlockSpec(memory_space=pl.ANY)
    vmem = pl.BlockSpec(memory_space=pltpu.VMEM)
    smem = pl.BlockSpec(memory_space=pltpu.SMEM)
    master = jax.ShapeDtypeStruct((LAYERS, ROWS, 1024), F32)
    dma = pltpu.SemaphoreType.DMA
    return pl.pallas_call(
        kernel,
        out_shape=(master, master, master, jax.ShapeDtypeStruct((512, 1024), BF)),
        in_specs=[any_space, smem, vmem, smem, vmem] + [any_space] * 4,
        out_specs=(any_space,) * 4,
        scratch_shapes=[
            pltpu.VMEM((LAYERS, ROWS, 1024), F32),
            pltpu.VMEM((LAYERS, ROWS, 1024), F32),
            pltpu.VMEM((LAYERS, ROWS, 1024), F32),
            pltpu.VMEM((LAYERS, ROWS, 1024), F32),
            pltpu.VMEM((LAYERS, 2, ROWS, HALF), BF),
            pltpu.VMEM((LAYERS, 2, 4, 4, ROWS, HALF), BF),
            pltpu.VMEM((4, 512, 1024), BF),
            pltpu.VMEM((2, 512, 1024), BF),
            pltpu.VMEM((2, CHUNKS, 4, 2, ROWS, HALF), BF),
            pltpu.VMEM((CHUNKS, 2, ROWS, HALF), F32),
            pltpu.VMEM((CHUNKS, 2, ROWS, HALF), BF),
            pltpu.VMEM((CHUNKS, 2, ROWS, HALF), BF),
            pltpu.VMEM((2, 2 * ROWS, HALF), F32),
            pltpu.VMEM((4, ROWS, 1024), F32),
            pltpu.VMEM((STEPS - 4, 8, 8, 2 * ROWS), F32),
            pltpu.VMEM((CHUNKS, 2, ROWS, HALF), BF),
            pltpu.VMEM((128, 2048), BF),
            pltpu.VMEM((CHUNKS, 2, ROWS, 1), F32),
            pltpu.VMEM((CHUNKS, 8, 128), F32),
            pltpu.VMEM((CHUNKS, 8, 128), F32),
            pltpu.VMEM((3, 8, 8, 128), F32),
            dma((LAYERS, 4)),
            dma((LAYERS, 3)),
            dma((4,)),
            dma((3, 7)),
            dma((3, 7)),
            dma((LAYERS, 2)),
            dma((LAYERS, 2)),
            dma((LAYERS, 24)),
            dma((LAYERS, 24)),
            dma((3,)),
            dma((3,)),
            dma((4,)),
            dma((4,)),
            dma((8,)),
            dma((8,)),
            dma((8,)),
            dma((8,)),
            dma((8,)),
            dma((8,)),
            dma((8, 8)),
            dma((8, 8)),
            dma((CHUNKS, 2)),
            dma((CHUNKS, 2)),
        ],
        compiler_params=pltpu.CompilerParams(
            collective_id=0, has_side_effects=True, vmem_limit_bytes=64 * 1024 * 1024 - 65536
        ),
    )(
        tokens,
        counts.reshape(1, 1),
        patch_index.reshape(512, 1),
        clip_limit.reshape(1, 1),
        norm_gain.reshape(32, HALF),
        params,
        moments,
        seconds,
        gradients,
    )


def solution(mesh):
    shard = P(None, "dp", "fsdp")
    return jax.shard_map(
        per_device,
        mesh=mesh,
        in_specs=(P("dp", None), P("dp"), P("dp"), P(), P(), shard, shard, shard, shard),
        out_specs=(shard, shard, shard, P("dp", "fsdp")),
        check_vma=False,
    )
```

```python
import functools
import math

import jax
import jax.numpy as jnp
from jax import lax
from jax.experimental import pallas as pl
from jax.experimental.pallas import tpu as pltpu
from jax.sharding import PartitionSpec as P

D = 4096
LAYERS = 4
STEP = 40
ROWS = 128
HALF = 512
CHUNKS = 4
STEPS = LAYERS * CHUNKS

beta_one = 0.9
beta_two = 0.95
adam_eps = 1e-08
learning_rate = 0.0024
weight_decay = 0.05
norm_eps = 1e-06
BF = jnp.bfloat16
F32 = jnp.float32
MESH = pl.DeviceIdType.MESH


def kernel(
    tokens_hbm, counts_ref, patch_hbm, clip_ref, gain_hbm, params_hbm, moments_hbm, seconds_hbm,
    gradients_hbm, params_out, moments_out, seconds_out, mixed_out,
    pv, mv, vv, gv, wb, tok, oth, xbuf, stream, ysend, yrecv, acc, statbuf,
    table, valid, meta_s, meta_r, red, patch_ref, gain_raw, gain_ref,
    in_sem, out_sem, tok_sem, small_sem, red_s, red_r, wx_s, wx_r, ag_s, ag_r, ts_s, ts_r,
    y_s, y_r, yl_s, yl_r, xd_s, xd_r, xi_s, xi_r, f_s, f_r, st_s, st_r, fin_s, fin_r,
):
    dp = lax.axis_index("dp")
    fs = lax.axis_index("fsdp")
    x = dp % 4
    y = (dp // 4) % 4
    zh = dp // 16
    zl = fs // 2
    c = fs % 2
    b = zh
    a = (zl + zh) % 2
    mine = 2 * a + c

    def flip(v, bit):
        return 1 - v if bit else v

    def at(xx, yy, hh, ll, cc):
        return (hh * 16 + yy * 4 + xx, ll * 2 + cc)

    def along_x(d):
        return at((x + d) % 4, y, zh, zl, c)

    def along_y(d):
        return at(x, (y + d) % 4, zh, zl, c)

    def column(r):
        return at(x, y, flip(zh, r & 4), flip(zl, r & 2), flip(c, r & 1))

    def block_of(r):
        return 2 * flip(a, r & 2) + flip(c, r & 1)

    core_peer = column(1)
    x_peer = column(2)
    y_peer = column(6)

    def remote(src, dst, ssem, rsem, dev):
        return pltpu.make_async_remote_copy(
            src_ref=src, dst_ref=dst, send_sem=ssem, recv_sem=rsem, device_id=dev,
            device_id_type=MESH,
        )

    for l in range(LAYERS):
        for h in range(2):
            pltpu.make_async_copy(
                gradients_hbm.at[l, :, pl.ds(HALF * h, HALF)], gv.at[l, h], in_sem.at[l, 1]
            ).start()
    barrier = pltpu.get_barrier_semaphore()
    plane = [
        at((x + i) % 4, (y + j) % 4, zh, zl, c) for j in range(4) for i in range(4) if i or j
    ]
    others = plane + [column(r) for r in range(1, 8)]
    for dev in others:
        pl.semaphore_signal(barrier, inc=1, device_id=dev, device_id_type=MESH)
    for l in range(LAYERS):
        for src, dst in ((params_hbm, pv), (moments_hbm, mv), (seconds_hbm, vv)):
            pltpu.make_async_copy(src.at[l], dst.at[l], in_sem.at[l, 0]).start()
    for q in range(4):
        pltpu.make_async_copy(
            tokens_hbm.at[:, pl.ds(1024 * q, 1024)], tok.at[q], tok_sem.at[0]
        ).start()
    small = [pltpu.make_async_copy(gain_hbm, gain_raw, small_sem.at[0])]
    for k in range(CHUNKS):
        small.append(
            pltpu.make_async_copy(
                patch_hbm.at[pl.ds(ROWS * k, ROWS)], patch_ref.at[k], small_sem.at[1]
            )
        )
    for copy in small:
        copy.start()

    total = jnp.zeros((8, HALF), F32)
    for l in range(LAYERS):
        pltpu.make_async_copy(gv.at[l], gv.at[l], in_sem.at[l, 1]).wait()

        def squares(i, part, l=l):
            for h in range(2):
                g = gv[l, h, pl.ds(pl.multiple_of(i * 32, 32), 32), :]
                g = g * g
                part = part + ((g[0:8] + g[8:16]) + (g[16:24] + g[24:32]))
            return part

        total = lax.fori_loop(0, 4, squares, total)
    tile = total[:, 0:128]
    for i in range(1, 4):
        tile = tile + total[:, 128 * i : 128 * (i + 1)]
    with jax.named_scope("barrier"):
        pl.semaphore_wait(barrier, len(others))

    def exchange(stage, devs, tile, filler):
        red[stage, 0] = tile
        copies = [
            remote(
                red.at[stage, 0], red.at[stage, r + 1], red_s.at[stage], red_r.at[stage], dev
            )
            for r, dev in enumerate(devs)
        ]
        for copy in copies:
            copy.start()
        filler()
        with jax.named_scope("reduce_wait"):
            came = red.at[stage, pl.ds(1, len(devs))]
            pltpu.make_async_copy(came, came, red_s.at[stage]).wait()
            pltpu.make_async_copy(came, came, red_r.at[stage]).wait()
            for r in range(len(devs)):
                tile = tile + red[stage, r + 1]
        return tile

    def token_copy(i):
        rows = pl.ds(256 * i, 256)
        return remote(
            tok.at[2 * (1 - b) + c, rows], oth.at[c, rows], ts_s.at[i], ts_r.at[i], y_peer
        )

    def fill_column():
        pltpu.make_async_copy(tok, tok, tok_sem.at[0]).wait()
        token_copy(0).start()
        token_copy(1).start()

    def fill_table():
        lane = lax.broadcasted_iota(jnp.int32, (16, 1024), 1).astype(F32)
        row = lax.broadcasted_iota(jnp.int32, (16, 1024), 0).astype(F32)
        angle = row * jnp.exp(lane * (-math.log(10000.0) / 1024.0))
        for q, wave in ((0, jnp.sin(angle)), (1, jnp.cos(angle))):
            cols = slice(1024 * q, 1024 * (q + 1))
            for i in range(3):
                piece = wave.astype(BF)
                table[16 * i : 16 * (i + 1), cols] = piece
                wave = wave - piece.astype(F32)
        table[48:128, :] = jnp.zeros((80, 2048), BF)
        small[0].wait()
        pltpu.make_async_copy(patch_ref, patch_ref, small_sem.at[1]).wait()
        for l in range(LAYERS):
            for i in range(8):
                gain_ref[8 * l + i : 8 * l + i + 1, :] = gain_raw[
                    l : l + 1, HALF * i : HALF * (i + 1)
                ]

    tile = exchange(0, [column(r) for r in range(1, 8)], tile, fill_column)
    tile = exchange(1, plane, tile, fill_table)
    norm = jnp.sqrt(jnp.sum(jnp.sum(tile, axis=1, keepdims=True), axis=0, keepdims=True))
    factor = jnp.minimum(1.0, clip_ref[0, 0] / (norm + 1e-06))

    def weight_copies(l):
        here = wb.at[l, zl, y, x]
        keep = pltpu.make_async_copy(ysend.at[l, c], here, wx_s.at[l, 1])
        give = remote(ysend.at[l, 1 - c], here, wx_s.at[l, 0], wx_r.at[l, 0], core_peer)
        same = remote(ysend.at[l, c], here, wx_s.at[l, 0], wx_r.at[l, 1], x_peer)
        cross = remote(ysend.at[l, 1 - c], here, wx_s.at[l, 1], wx_r.at[l, 1], column(3))
        return keep, give, same, cross

    for l in range(LAYERS):
        three = pv.at[pl.ds(0, 3)]
        pltpu.make_async_copy(three, three, in_sem.at[l, 0]).wait()

        def update(i, _, l=l):
            rows = pl.ds(pl.multiple_of(i * 16, 16), 16)
            p = pv[l, rows, :]
            clipped = jnp.concatenate([gv[l, 0, rows, :], gv[l, 1, rows, :]], axis=1) * factor
            m = beta_one * mv[l, rows, :] + (1.0 - beta_one) * clipped
            v = beta_two * vv[l, rows, :] + (1.0 - beta_two) * clipped * clipped
            root = jnp.sqrt(v * (1.0 / (1.0 - beta_two**STEP))) + adam_eps
            direction = (m * (1.0 / (1.0 - beta_one**STEP))) / root
            p = p - learning_rate * (direction + weight_decay * p)
            mv[l, rows, :] = m
            vv[l, rows, :] = v
            pv[l, rows, :] = p
            w = p.astype(BF)
            ysend[l, 0, rows, :] = w[:, 0:HALF]
            ysend[l, 1, rows, :] = w[:, HALF:]
            return 0

        with jax.named_scope("update"):
            lax.fori_loop(0, ROWS // 16, update, 0)
        own, give_core, same, cross = weight_copies(l)

        @pl.when(c == a)
        def _():
            own.start()
            give_core.start()

        @pl.when(c != a)
        def _():
            same.start()
            cross.start()

    def weights_kept():
        for l in range(LAYERS):

            @pl.when(c == a)
            def _(l=l):
                weight_copies(l)[0].wait()

    def weights_sent():
        for l in range(LAYERS):
            keep, give_core, same, cross = weight_copies(l)

            @pl.when(c == a)
            def _():
                give_core.wait_send()

            @pl.when(c != a)
            def _():
                same.wait_send()
                cross.wait_send()

    def start_outputs():
        for l in range(LAYERS):
            for j, (src, dst) in enumerate(((pv, params_out), (mv, moments_out), (vv, seconds_out))):
                pltpu.make_async_copy(src.at[l], dst.at[l], out_sem.at[j]).start()

    def piece(q, h, phase, xx, yy, part):
        l, nb = q // 2, (1 - b) + (q % 2) * (2 * b - 1)
        if phase == 0:
            return wb.at[l, nb, yy, xx, pl.ds(64 * h + 32 * part, 32), :]
        if h == 0:
            return wb.at[l, nb, yy, pl.ds(2 * part, 2), pl.ds(0, 64), :]
        return wb.at[l, nb, pl.ds(2 * part, 2), xx, pl.ds(64, 64), :]

    def gather_copy(q, h, phase, sign, kind):
        on_x = (h == 0) == (phase == 0)
        step = 1 if sign == 0 else 3
        part = sign if kind != 1 else 1 - sign
        xx, yy = x, y
        if kind == 2:
            if on_x:
                xx = (x + 4 - step) % 4
            else:
                yy = (y + 4 - step) % 4
        ref = piece(q, h, phase, xx, yy, part)
        group = 2 * phase + (0 if kind == 0 else 1)
        out = (2 * phase + 1) if kind == 2 else 2 * phase
        dev = along_x(step) if on_x else along_y(step)
        return remote(ref, ref, ag_s.at[q, out], ag_r.at[q, group], dev)

    def both(q, phase, kind):
        return [gather_copy(q, h, phase, sign, kind) for h in (0, 1) for sign in (0, 1)]

    def start_all(copies):
        for copy in copies:
            copy.start()

    def group_ref(q, group):
        l, nb = q // 2, q % 2
        if group < 2:
            return wb.at[l, nb, 0, pl.ds(0, group + 1)]
        return wb.at[l, nb, pl.ds(0, group - 1)]

    def recv_group(q, group):
        ref = group_ref(q, group)
        pltpu.make_async_copy(ref, ref, ag_r.at[q, group]).wait()

    def sent_group(q, group):
        ref = group_ref(q, group ^ 1)
        pltpu.make_async_copy(ref, ref, ag_s.at[q, group]).wait()

    def own_out(q):
        with jax.named_scope("own_out"):
            l, nb = q // 2, (1 - b) + (q % 2) * (2 * b - 1)
            here = wb.at[l, nb, y, x]

            @pl.when((c != a) | (nb != zl))
            def _():
                pltpu.make_async_copy(here, here, wx_r.at[l, (nb + zl) % 2]).wait()

            start_all(both(q, 0, 0))
            start_all(both(q, 0, 1))

    def own_on(q):
        with jax.named_scope("own_on"):
            recv_group(q, 0)
            start_all(both(q, 0, 2))

    def line_out(q):
        with jax.named_scope("line_out"):
            recv_group(q, 1)
            start_all(both(q, 1, 0))
            start_all(both(q, 1, 1))

    def line_on(q):
        with jax.named_scope("line_on"):
            recv_group(q, 2)
            start_all(both(q, 1, 2))

    def plane_done(q):
        with jax.named_scope("plane_done"):
            recv_group(q, 3)

    lane = lax.broadcasted_iota(jnp.int32, (ROWS, 128), 1)
    lane_f = lane.astype(F32)

    def spread(index):
        hit = (lane_f == index) | (lane_f == index + 16.0) | (lane_f == index + 32.0)
        return jnp.where(hit, 1.0, 0.0).astype(BF)

    def code(index, q):
        return jnp.dot(
            spread(index), table[:, 1024 * q : 1024 * (q + 1)], preferred_element_type=F32
        )

    def place(k, side, blocks, centre, scale):
        for q in range(2):
            for h in range(2):
                i = 2 * q + h
                values = blocks[i]
                gain = gain_ref[pl.ds(4 * b + i, 1), :]
                xbuf[0, k, i, side] = ((values - centre) * scale * gain).astype(BF)

                @pl.when(mine == i)
                def _(values=values):
                    stream[k, side] = values

    def embed_own(k):
        with jax.named_scope("embed_own"):
            rows = slice(ROWS * k, ROWS * (k + 1))
            p = jnp.broadcast_to(patch_ref[k : k + 1, :], (ROWS, 128)).T[:, 0:1]
            high = (p // 16).astype(F32)
            low = (p % 16).astype(F32)
            slot = lax.broadcasted_iota(jnp.int32, (ROWS, 1), 0) + ROWS * k
            real = jnp.where(slot < counts_ref[0], 1.0, 0.0)
            centre = jnp.zeros((ROWS, 1), F32)
            for q in range(4):
                values = tok[q, rows, :].astype(F32) + code(high if q < 2 else low, q % 2)
                values = jnp.where(real > 0.5, values, 0.0)
                gv[q, 0] = values[:, 0:HALF]
                gv[q, 1] = values[:, HALF:]
                centre = centre + jnp.sum(values, axis=1, keepdims=True)
            centre = centre * (1.0 / D)
            square = jnp.zeros((ROWS, 1), F32)
            for q in range(4):
                for h in range(2):
                    shifted = gv[q, h] - centre
                    square = square + jnp.sum(shifted * shifted, axis=1, keepdims=True)
            scale = lax.rsqrt(square * (1.0 / D) + norm_eps)
            place(k, zh, [gv[2 * b + i // 2, i % 2] for i in range(4)], centre, scale)
            valid[k, zh] = real
            cols = jnp.zeros((ROWS, 128), F32)
            for i, value in enumerate((centre, scale, high, low, real)):
                cols = jnp.where(lane == i, value, cols)
            meta_s[k] = cols.T[0:8, :]

    def meta_copy():
        return remote(meta_s, meta_r, ts_s.at[2], ts_r.at[2], y_peer)

    def share_copy(i):
        ref = oth.at[c, pl.ds(256 * i, 256)]
        return remote(ref, ref, ts_s.at[3 + i], ts_r.at[3 + i], core_peer)

    def embed_other(k):
        with jax.named_scope("embed_other"):
            rows = slice(ROWS * k, ROWS * (k + 1))
            cols = jnp.concatenate([meta_r[k]] * 16, axis=0).T
            centre, scale, high, low, real = [cols[:, i : i + 1] for i in range(5)]
            index = jnp.where(b == 0, high, low)
            blocks = []
            for q in range(2):
                values = oth[q, rows, :].astype(F32) + code(index, q)
                values = jnp.where(real > 0.5, values, 0.0)
                blocks += [values[:, 0:HALF], values[:, HALF:]]
            place(k, 1 - zh, blocks, centre, scale)
            valid[k, 1 - zh] = real

    def share(i):
        with jax.named_scope("token_wait"):
            token_copy(i).wait_recv()
        share_copy(i).start()

    def share(i):
        with jax.named_scope("token_wait"):
            token_copy(i).wait_recv()
        share_copy(i).start()

    def y_copy(k):
        return remote(ysend.at[k], yrecv.at[k], y_s.at[k], y_r.at[k], y_peer)

    def core_copy(s):
        ref = xbuf.at[(s // 4 + 1) % 2, s % 4, mine]
        return remote(ref, ref, xd_s.at[s % 8], xd_r.at[s % 8], core_peer)

    def chip_copy(s):
        ref = xbuf.at[(s // 4 + 1) % 2, s % 4, mine]
        return remote(ref, ref, xi_s.at[s % 8], xi_r.at[s % 8], x_peer)

    def pass_copy(s):
        ref = xbuf.at[(s // 4 + 1) % 2, s % 4, block_of(2)]
        return remote(ref, ref, f_s.at[s % 8], f_r.at[s % 8], core_peer)

    def stat_copies(s):
        return [
            remote(
                statbuf.at[s, 0], statbuf.at[s, r], st_s.at[s % 8], st_r.at[s % 8], column(r)
            )
            for r in range(1, 8)
        ]

    def final_place(k):
        return mixed_out.at[pl.ds(k * ROWS, ROWS), pl.ds(pl.multiple_of(c * HALF, HALF), HALF)]

    def final_copy(k):
        return remote(
            xbuf.at[0, k, 0, a], final_place(k), fin_s.at[k, 0], fin_r.at[k, c],
            at(x, y, zh, 1 - zl, a),
        )

    def final_core(k):
        return remote(
            xbuf.at[0, k, 0, 1 - a], final_place(k), fin_s.at[k, 1], fin_r.at[k, c], core_peer
        )

    def final_recv(k, part):
        dst = mixed_out.at[pl.ds(k * ROWS, ROWS), pl.ds(part * HALF, HALF)]
        return pltpu.make_async_copy(xbuf.at[0, k, 0, 0], dst, fin_r.at[k, part])

    def normalise(s):
        with jax.named_scope("normalise"):
            last = s - 4
            l, k = s // 4, s % 4
            means = [statbuf[last, r, 0:1, :] for r in range(8)]
            mean = means[0]
            for r in range(1, 8):
                mean = mean + means[r]
            mean = mean * 0.125
            spread_sum = jnp.zeros_like(mean)
            for r in range(8):
                off = means[r] - mean
                spread_sum = spread_sum + (statbuf[last, r, 1:2, :] + float(HALF) * off * off)
            scale = lax.rsqrt(spread_sum * (1.0 / D) + norm_eps)
            rows = jnp.concatenate([means[r] - mean for r in range(4)] + [scale] * 4, axis=0)
            cols = jnp.concatenate([rows] * 16, axis=0).T
            scale = cols[:, 4:5]
            for r in range(4):
                i = block_of(r)
                off = cols[:, r : r + 1]
                gain = gain_ref[pl.ds(8 * l + 4 * b + i, 1), :]
                d = xbuf[l % 2, k, i].reshape(2 * ROWS, HALF).astype(F32)
                xbuf[l % 2, k, i] = ((d + off) * scale * gain).astype(BF).reshape(2, ROWS, HALF)

    def product(s, h):
        l, k = s // 4, s % 4
        with jax.named_scope("product"):
            left = jnp.concatenate(
                [xbuf[l % 2, k, i].reshape(2 * ROWS, HALF) for i in range(4)], axis=1
            )

            def column_tile(n, _):
                cols = pl.ds(pl.multiple_of(n * 256, 256), 256)
                right = wb[l, h, :, :, :, cols].reshape(2048, 256)
                tile = jnp.dot(left, right, preferred_element_type=F32)
                acc[:, :, cols] = tile.reshape(2, ROWS, 256)
                return 0

            lax.fori_loop(0, 2, column_tile, 0)

    def last_copy(k, i):
        return remote(ysend.at[k, i], yrecv.at[k, i], yl_s.at[k, i], yl_r.at[k, i], y_peer)

    def give(s):
        k = s % 4
        product(s, 1 - b)

        @pl.when(s < STEPS - 4)
        def _():
            ysend[k] = acc[...].astype(BF)
            y_copy(k).start()

        @pl.when(s >= STEPS - 4)
        def _():
            ysend[k, 0] = acc[1 - b].astype(BF)
            last_copy(k, 0).start()
            gv[k, 0] = acc[b]

    def receive(s):
        k = s % 4
        product(s, b)
        with jax.named_scope("y_wait"):
            y_copy(k).wait_recv()
        with jax.named_scope("receive"):
            values = (stream[k] + acc[...] + yrecv[k].astype(F32)).reshape(2 * ROWS, HALF)
            stream[k] = values.reshape(2, ROWS, HALF)
            mean = jnp.sum(values, axis=1, keepdims=True) * (1.0 / HALF)
            d = values - mean
            square = jnp.sum(d * d, axis=1, keepdims=True)
            lanes = lax.broadcasted_iota(jnp.int32, (2 * ROWS, 128), 1)
            cols = jnp.where(lanes == 0, mean, jnp.where(lanes == 1, square, 0.0))
            statbuf[s, 0] = cols.T[0:2, :]
            xbuf[(s // 4 + 1) % 2, k, mine] = d.astype(BF).reshape(2, ROWS, HALF)
            start_all(stat_copies(s))
            chip_copy(s).start()
            core_copy(s).start()

    def give_rest(s):
        k = s % 4
        product(s, b)
        ysend[k, 1] = (acc[1 - b] + stream[k, 1 - b]).astype(BF)
        last_copy(k, 1).start()
        gv[k, 1] = acc[b] + stream[k, b]

    def finish(s, i):
        k = s % 4
        with jax.named_scope("y_wait"):
            last_copy(k, 1 - i).wait_recv()
        with jax.named_scope("finish"):
            real = valid[k, zh] > 0.5
            values = gv[k, i] + yrecv[k, 1 - i].astype(F32)
            xbuf[0, k, 0, i] = jnp.where(real, values, 0.0).astype(BF)

    def finish_both(s):
        k = s % 4
        finish(s, a)
        final_copy(k).start()
        finish(s, 1 - a)

        @pl.when(c == a)
        def _():
            dst = final_place(k)
            pltpu.make_async_copy(xbuf.at[0, k, 0, 1 - a], dst, fin_r.at[k, c]).start()

        @pl.when(c != a)
        def _():
            final_core(k).start()

    def body(s, _):
        @pl.when((s >= 4) & (s < STEPS))
        def _():
            with jax.named_scope("chip_wait"):
                chip_copy(s - 4).wait_recv()
            pass_copy(s - 4).start()

        @pl.when(s < STEPS - 2)
        def _():
            @pl.when(s % 4 == 2)
            def _():
                plane_done((s - 2) // 2 + 1)

            receive(s - 2)

        @pl.when((s == STEPS - 3) | (s == STEPS - 2))
        def _():
            @pl.when(s == STEPS - 3)
            def _():
                plane_done(2 * LAYERS - 1)

            give_rest(s - 1)

        @pl.when(s >= STEPS - 1)
        def _():
            finish_both(s - 3)

        @pl.when((s >= 4) & (s < STEPS))
        def _():
            last = s - 4
            with jax.named_scope("stat_wait"):
                y_copy(s % 4).wait_send()
                seven = statbuf.at[last, pl.ds(1, 7)]
                pltpu.make_async_copy(seven, seven, st_s.at[last % 8]).wait()
                pltpu.make_async_copy(seven, seven, st_r.at[last % 8]).wait()
            with jax.named_scope("block_wait"):
                core_copy(last).wait()
                chip_copy(last).wait_send()
                pass_copy(last).wait()
            normalise(s)

            @pl.when(s % 4 == 0)
            def _():
                plane_done(s // 2)

            late = s >= STEPS - 2

            @pl.when(late & (a == 0))
            def _():
                give_rest(s)

            give(s)

            @pl.when(late & (a == 1))
            def _():
                give_rest(s)

        @pl.when((s % 2 == 0) & (s < STEPS - 2))
        def _():
            line_on(s // 2 + 1)

        @pl.when((s % 2 == 1) & (s < STEPS - 3))
        def _():
            q = (s + 1) // 2
            line_out(q + 1)

            @pl.when(q + 2 < 2 * LAYERS)
            def _():
                own_on(q + 2)

            @pl.when(q + 3 < 2 * LAYERS)
            def _():
                own_out(q + 3)

        return 0

    weights_kept()
    own_out(0)
    embed_own(0)
    own_on(0)
    own_out(1)
    embed_own(1)
    line_out(0)
    embed_own(2)
    embed_own(3)
    meta_copy().start()
    start_outputs()
    line_on(0)
    own_on(1)
    own_out(2)
    share(0)
    with jax.named_scope("meta_wait"):
        meta_copy().wait_recv()
        share_copy(0).wait_recv()
    embed_other(0)
    share(1)
    plane_done(0)
    weights_sent()
    give(0)
    line_out(1)
    own_on(2)
    own_out(3)
    embed_other(1)
    give(1)
    line_on(1)
    with jax.named_scope("share_wait"):
        share_copy(1).wait_recv()
    embed_other(2)
    give(2)
    embed_other(3)
    give(3)
    line_out(2)
    own_on(3)
    own_out(4)
    lax.fori_loop(2, STEPS + 3, body, 0)

    for k in range(CHUNKS):
        with jax.named_scope("final_wait"):
            for part in (0, 1):
                final_recv(k, part).wait()
        for i in range(2):
            last_copy(k, i).wait_send()
        final_copy(k).wait_send()

        @pl.when(c != a)
        def _(k=k):
            final_core(k).wait_send()

    with jax.named_scope("end_wait"):
        meta_copy().wait_send()
    for i in range(2):
        token_copy(i).wait_send()
        share_copy(i).wait_send()
    def sent(q, _):
        for group in range(4):
            sent_group(q, group)
        return 0

    with jax.named_scope("end_sent"):
        lax.fori_loop(0, 2 * LAYERS, sent, 0)
    for j, dst in enumerate((pv, mv, vv)):
        pltpu.make_async_copy(dst, dst, out_sem.at[j]).wait()


def hand_over(p, m, v, mixed, p_out, m_out, v_out, mixed_out, sem):
    copies = [
        pltpu.make_async_copy(src, dst, sem.at[j])
        for j, (src, dst) in enumerate(((p, p_out), (m, m_out), (v, v_out), (mixed, mixed_out)))
    ]
    for copy in copies:
        copy.start()
    for copy in copies:
        copy.wait()


def per_device(
    tokens, counts, patch_index, clip_limit, norm_gain, params, moments, seconds, gradients
):
    any_space = pl.BlockSpec(memory_space=pl.ANY)
    hbm = pl.BlockSpec(memory_space=pltpu.HBM)
    smem = pl.BlockSpec(memory_space=pltpu.SMEM)
    master = jax.ShapeDtypeStruct((LAYERS, ROWS, 1024), F32)
    dma = pltpu.SemaphoreType.DMA
    shapes = (master, master, master, jax.ShapeDtypeStruct((512, 1024), BF))
    results = pl.pallas_call(
        kernel,
        out_shape=shapes,
        in_specs=[hbm, smem, hbm, smem, hbm] + [hbm] * 4,
        out_specs=(any_space,) * 4,
        scratch_shapes=[
            pltpu.VMEM((LAYERS, ROWS, 1024), F32),
            pltpu.VMEM((LAYERS, ROWS, 1024), F32),
            pltpu.VMEM((LAYERS, ROWS, 1024), F32),
            pltpu.VMEM((LAYERS, 2, ROWS, HALF), F32),
            pltpu.VMEM((LAYERS, 2, 4, 4, ROWS, HALF), BF),
            pltpu.VMEM((4, 512, 1024), BF),
            pltpu.VMEM((2, 512, 1024), BF),
            pltpu.VMEM((2, CHUNKS, 4, 2, ROWS, HALF), BF),
            pltpu.VMEM((CHUNKS, 2, ROWS, HALF), F32),
            pltpu.VMEM((CHUNKS, 2, ROWS, HALF), BF),
            pltpu.VMEM((CHUNKS, 2, ROWS, HALF), BF),
            pltpu.VMEM((2, ROWS, HALF), F32),
            pltpu.VMEM((STEPS - 4, 8, 2, 2 * ROWS), F32),
            pltpu.VMEM((128, 2048), BF),
            pltpu.VMEM((CHUNKS, 2, ROWS, 1), F32),
            pltpu.VMEM((CHUNKS, 8, 128), F32),
            pltpu.VMEM((CHUNKS, 8, 128), F32),
            pltpu.VMEM((2, 16, 8, 128), F32),
            pltpu.VMEM((CHUNKS, 128), jnp.int32),
            pltpu.VMEM((LAYERS, D), F32),
            pltpu.VMEM((32, HALF), F32),
            dma((LAYERS, 2)),
            dma((3,)),
            dma((1,)),
            dma((2,)),
            dma((2,)),
            dma((2,)),
            dma((LAYERS, 2)),
            dma((LAYERS, 2)),
            dma((2 * LAYERS, 4)),
            dma((2 * LAYERS, 4)),
            dma((5,)),
            dma((5,)),
            dma((4,)),
            dma((4,)),
            dma((CHUNKS, 2)),
            dma((CHUNKS, 2)),
            dma((8,)),
            dma((8,)),
            dma((8,)),
            dma((8,)),
            dma((8,)),
            dma((8,)),
            dma((8,)),
            dma((8,)),
            dma((CHUNKS, 2)),
            dma((CHUNKS, 2)),
        ],
        compiler_params=pltpu.CompilerParams(
            collective_id=0, has_side_effects=True, vmem_limit_bytes=49200000
        ),
    )(
        tokens,
        counts,
        pltpu.with_memory_space_constraint(patch_index, pltpu.HBM),
        clip_limit.reshape(1, 1),
        pltpu.with_memory_space_constraint(norm_gain, pltpu.HBM),
        params,
        moments,
        seconds,
        gradients,
    )
    return pl.pallas_call(
        hand_over,
        out_shape=shapes,
        in_specs=[any_space] * 4,
        out_specs=(any_space,) * 4,
        scratch_shapes=[
            dma((4,)),
        ],
        compiler_params=pltpu.CompilerParams(vmem_limit_bytes=1024 * 1024),
    )(*results)


def solution(mesh):
    shard = P(None, "dp", "fsdp")
    return jax.shard_map(
        per_device,
        mesh=mesh,
        in_specs=(P("dp", None), P("dp"), P("dp"), P(), P(), shard, shard, shard, shard),
        out_specs=(shard, shard, shard, P("dp", "fsdp")),
        check_vma=False,
    )
```

```python
import functools
import math

import jax
import jax.numpy as jnp
from jax import lax
from jax.experimental import pallas as pl
from jax.experimental.pallas import tpu as pltpu
from jax.sharding import PartitionSpec as P

D = 4096
LAYERS = 4
STEP = 40
ROWS = 128
HALF = 512
CHUNKS = 4
STEPS = LAYERS * CHUNKS

beta_one = 0.9
beta_two = 0.95
adam_eps = 1e-08
learning_rate = 0.0024
weight_decay = 0.05
norm_eps = 1e-06
BF = jnp.bfloat16
F32 = jnp.float32
MESH = pl.DeviceIdType.MESH


def kernel(
    tokens_hbm, counts_ref, patch_hbm, clip_ref, gain_hbm, params_hbm, moments_hbm, seconds_hbm,
    gradients_hbm, params_out, moments_out, seconds_out, mixed_out,
    pv, mv, vv, gv, wb, tok, oth, xbuf, stream, ysend, yrecv, acc, statbuf,
    table, valid, meta_s, meta_r, red, patch_ref, gain_raw, gain_ref,
    in_sem, out_sem, tok_sem, small_sem, red_s, red_r, wx_s, wx_r, ag_s, ag_r, ts_s, ts_r,
    y_s, y_r, yl_s, yl_r, xd_s, xd_r, xi_s, xi_r, f_s, f_r, st_s, st_r, fin_s, fin_r,
):
    dp = lax.axis_index("dp")
    fs = lax.axis_index("fsdp")
    x = dp % 4
    y = (dp // 4) % 4
    zh = dp // 16
    zl = fs // 2
    c = fs % 2
    b = zh
    a = (zl + zh) % 2
    mine = 2 * a + c

    def flip(v, bit):
        return 1 - v if bit else v

    def at(xx, yy, hh, ll, cc):
        return (hh * 16 + yy * 4 + xx, ll * 2 + cc)

    def along_x(d):
        return at((x + d) % 4, y, zh, zl, c)

    def along_y(d):
        return at(x, (y + d) % 4, zh, zl, c)

    def column(r):
        return at(x, y, flip(zh, r & 4), flip(zl, r & 2), flip(c, r & 1))

    def block_of(r):
        return 2 * flip(a, r & 2) + flip(c, r & 1)

    core_peer = column(1)
    x_peer = column(2)
    y_peer = column(6)

    def remote(src, dst, ssem, rsem, dev):
        return pltpu.make_async_remote_copy(
            src_ref=src, dst_ref=dst, send_sem=ssem, recv_sem=rsem, device_id=dev,
            device_id_type=MESH,
        )

    for l in range(LAYERS):
        for h in range(2):
            pltpu.make_async_copy(
                gradients_hbm.at[l, :, pl.ds(HALF * h, HALF)], gv.at[l, h], in_sem.at[l, 1]
            ).start()
    barrier = pltpu.get_barrier_semaphore()
    plane = [
        at((x + i) % 4, (y + j) % 4, zh, zl, c) for j in range(4) for i in range(4) if i or j
    ]
    others = plane + [column(r) for r in range(1, 8)]
    for dev in others:
        pl.semaphore_signal(barrier, inc=1, device_id=dev, device_id_type=MESH)
    for l in range(LAYERS):
        for src, dst in ((params_hbm, pv), (moments_hbm, mv), (seconds_hbm, vv)):
            pltpu.make_async_copy(src.at[l], dst.at[l], in_sem.at[l, 0]).start()
    for q in range(4):
        pltpu.make_async_copy(
            tokens_hbm.at[:, pl.ds(1024 * q, 1024)], tok.at[q], tok_sem.at[0]
        ).start()
    small = [pltpu.make_async_copy(gain_hbm, gain_raw, small_sem.at[0])]
    for k in range(CHUNKS):
        small.append(
            pltpu.make_async_copy(
                patch_hbm.at[pl.ds(ROWS * k, ROWS)], patch_ref.at[k], small_sem.at[1]
            )
        )
    for copy in small:
        copy.start()

    total = jnp.zeros((8, HALF), F32)
    for l in range(LAYERS):
        pltpu.make_async_copy(gv.at[l], gv.at[l], in_sem.at[l, 1]).wait()

        def squares(i, part, l=l):
            for h in range(2):
                g = gv[l, h, pl.ds(pl.multiple_of(i * 32, 32), 32), :]
                g = g * g
                part = part + ((g[0:8] + g[8:16]) + (g[16:24] + g[24:32]))
            return part

        total = lax.fori_loop(0, 4, squares, total)
    tile = total[:, 0:128]
    for i in range(1, 4):
        tile = tile + total[:, 128 * i : 128 * (i + 1)]
    with jax.named_scope("barrier"):
        pl.semaphore_wait(barrier, len(others))

    def exchange(stage, devs, tile, filler):
        red[stage, 0] = tile
        copies = [
            remote(
                red.at[stage, 0], red.at[stage, r + 1], red_s.at[stage], red_r.at[stage], dev
            )
            for r, dev in enumerate(devs)
        ]
        for copy in copies:
            copy.start()
        filler()
        with jax.named_scope("reduce_wait"):
            came = red.at[stage, pl.ds(1, len(devs))]
            pltpu.make_async_copy(came, came, red_s.at[stage]).wait()
            pltpu.make_async_copy(came, came, red_r.at[stage]).wait()
            for r in range(len(devs)):
                tile = tile + red[stage, r + 1]
        return tile

    def token_copy(i):
        rows = pl.ds(256 * i, 256)
        return remote(
            tok.at[2 * (1 - b) + c, rows], oth.at[c, rows], ts_s.at[i], ts_r.at[i], y_peer
        )

    def fill_column():
        pltpu.make_async_copy(tok, tok, tok_sem.at[0]).wait()
        token_copy(0).start()
        token_copy(1).start()

    def fill_table():
        lane = lax.broadcasted_iota(jnp.int32, (16, 1024), 1).astype(F32)
        row = lax.broadcasted_iota(jnp.int32, (16, 1024), 0).astype(F32)
        angle = row * jnp.exp(lane * (-math.log(10000.0) / 1024.0))
        for q, wave in ((0, jnp.sin(angle)), (1, jnp.cos(angle))):
            cols = slice(1024 * q, 1024 * (q + 1))
            for i in range(3):
                piece = wave.astype(BF)
                table[16 * i : 16 * (i + 1), cols] = piece
                wave = wave - piece.astype(F32)
        table[48:128, :] = jnp.zeros((80, 2048), BF)
        small[0].wait()
        pltpu.make_async_copy(patch_ref, patch_ref, small_sem.at[1]).wait()
        for l in range(LAYERS):
            for i in range(8):
                gain_ref[8 * l + i : 8 * l + i + 1, :] = gain_raw[
                    l : l + 1, HALF * i : HALF * (i + 1)
                ]

    tile = exchange(0, [column(r) for r in range(1, 8)], tile, fill_column)
    tile = exchange(1, plane, tile, fill_table)
    norm = jnp.sqrt(jnp.sum(jnp.sum(tile, axis=1, keepdims=True), axis=0, keepdims=True))
    factor = jnp.minimum(1.0, clip_ref[0, 0] / (norm + 1e-06))

    def weight_copies(l):
        here = wb.at[l, zl, y, x]
        keep = pltpu.make_async_copy(ysend.at[l, c], here, wx_s.at[l, 1])
        give = remote(ysend.at[l, 1 - c], here, wx_s.at[l, 0], wx_r.at[l, 0], core_peer)
        same = remote(ysend.at[l, c], here, wx_s.at[l, 0], wx_r.at[l, 1], x_peer)
        cross = remote(ysend.at[l, 1 - c], here, wx_s.at[l, 1], wx_r.at[l, 1], column(3))
        return keep, give, same, cross

    for l in range(LAYERS):
        three = pv.at[pl.ds(0, 3)]
        pltpu.make_async_copy(three, three, in_sem.at[l, 0]).wait()

        def update(i, _, l=l):
            rows = pl.ds(pl.multiple_of(i * 16, 16), 16)
            p = pv[l, rows, :]
            clipped = jnp.concatenate([gv[l, 0, rows, :], gv[l, 1, rows, :]], axis=1) * factor
            m = beta_one * mv[l, rows, :] + (1.0 - beta_one) * clipped
            v = beta_two * vv[l, rows, :] + (1.0 - beta_two) * clipped * clipped
            root = jnp.sqrt(v * (1.0 / (1.0 - beta_two**STEP))) + adam_eps
            direction = (m * (1.0 / (1.0 - beta_one**STEP))) / root
            p = p - learning_rate * (direction + weight_decay * p)
            mv[l, rows, :] = m
            vv[l, rows, :] = v
            pv[l, rows, :] = p
            w = p.astype(BF)
            ysend[l, 0, rows, :] = w[:, 0:HALF]
            ysend[l, 1, rows, :] = w[:, HALF:]
            return 0

        with jax.named_scope("update"):
            lax.fori_loop(0, ROWS // 16, update, 0)
        own, give_core, same, cross = weight_copies(l)

        @pl.when(c == a)
        def _():
            own.start()
            give_core.start()

        @pl.when(c != a)
        def _():
            same.start()
            cross.start()

    def weights_kept():
        for l in range(LAYERS):

            @pl.when(c == a)
            def _(l=l):
                weight_copies(l)[0].wait()

    def weights_sent():
        for l in range(LAYERS):
            keep, give_core, same, cross = weight_copies(l)

            @pl.when(c == a)
            def _():
                give_core.wait_send()

            @pl.when(c != a)
            def _():
                same.wait_send()
                cross.wait_send()

    def start_outputs():
        for l in range(LAYERS):
            for j, (src, dst) in enumerate(((pv, params_out), (mv, moments_out), (vv, seconds_out))):
                pltpu.make_async_copy(src.at[l], dst.at[l], out_sem.at[j]).start()

    def piece(q, h, phase, xx, yy, part):
        l, nb = q // 2, (1 - b) + (q % 2) * (2 * b - 1)
        if phase == 0:
            return wb.at[l, nb, yy, xx, pl.ds(64 * h + 32 * part, 32), :]
        if h == 0:
            return wb.at[l, nb, yy, pl.ds(2 * part, 2), pl.ds(0, 64), :]
        return wb.at[l, nb, pl.ds(2 * part, 2), xx, pl.ds(64, 64), :]

    def gather_copy(q, h, phase, sign, kind):
        on_x = (h == 0) == (phase == 0)
        step = 1 if sign == 0 else 3
        part = sign if kind != 1 else 1 - sign
        xx, yy = x, y
        if kind == 2:
            if on_x:
                xx = (x + 4 - step) % 4
            else:
                yy = (y + 4 - step) % 4
        ref = piece(q, h, phase, xx, yy, part)
        group = 2 * phase + (0 if kind == 0 else 1)
        out = (2 * phase + 1) if kind == 2 else 2 * phase
        dev = along_x(step) if on_x else along_y(step)
        return remote(ref, ref, ag_s.at[q, out], ag_r.at[q, group], dev)

    def both(q, phase, kind):
        return [gather_copy(q, h, phase, sign, kind) for h in (0, 1) for sign in (0, 1)]

    def start_all(copies):
        for copy in copies:
            copy.start()

    def group_ref(q, group):
        l, nb = q // 2, q % 2
        if group < 2:
            return wb.at[l, nb, 0, pl.ds(0, group + 1)]
        return wb.at[l, nb, pl.ds(0, group - 1)]

    def recv_group(q, group):
        ref = group_ref(q, group)
        pltpu.make_async_copy(ref, ref, ag_r.at[q, group]).wait()

    def sent_group(q, group):
        ref = group_ref(q, group ^ 1)
        pltpu.make_async_copy(ref, ref, ag_s.at[q, group]).wait()

    def own_out(q):
        with jax.named_scope("own_out"):
            l, nb = q // 2, (1 - b) + (q % 2) * (2 * b - 1)
            here = wb.at[l, nb, y, x]

            @pl.when((c != a) | (nb != zl))
            def _():
                pltpu.make_async_copy(here, here, wx_r.at[l, (nb + zl) % 2]).wait()

            start_all(both(q, 0, 0))
            start_all(both(q, 0, 1))

    def own_on(q):
        with jax.named_scope("own_on"):
            recv_group(q, 0)
            start_all(both(q, 0, 2))

    def line_out(q):
        with jax.named_scope("line_out"):
            recv_group(q, 1)
            start_all(both(q, 1, 0))
            start_all(both(q, 1, 1))

    def line_on(q):
        with jax.named_scope("line_on"):
            recv_group(q, 2)
            start_all(both(q, 1, 2))

    def plane_done(q):
        with jax.named_scope("plane_done"):
            recv_group(q, 3)

    lane = lax.broadcasted_iota(jnp.int32, (ROWS, 128), 1)
    lane_f = lane.astype(F32)

    def spread(index):
        hit = (lane_f == index) | (lane_f == index + 16.0) | (lane_f == index + 32.0)
        return jnp.where(hit, 1.0, 0.0).astype(BF)

    def code(index, q):
        return jnp.dot(
            spread(index), table[:, 1024 * q : 1024 * (q + 1)], preferred_element_type=F32
        )

    def place(k, side, blocks, centre, scale):
        for q in range(2):
            for h in range(2):
                i = 2 * q + h
                values = blocks[i]
                gain = gain_ref[pl.ds(4 * b + i, 1), :]
                xbuf[0, k, i, side] = ((values - centre) * scale * gain).astype(BF)

                @pl.when(mine == i)
                def _(values=values):
                    stream[k, side] = values

    def embed_own(k):
        with jax.named_scope("embed_own"):
            rows = slice(ROWS * k, ROWS * (k + 1))
            p = jnp.broadcast_to(patch_ref[k : k + 1, :], (ROWS, 128)).T[:, 0:1]
            high = (p // 16).astype(F32)
            low = (p % 16).astype(F32)
            slot = lax.broadcasted_iota(jnp.int32, (ROWS, 1), 0) + ROWS * k
            real = jnp.where(slot < counts_ref[0], 1.0, 0.0)
            centre = jnp.zeros((ROWS, 1), F32)
            for q in range(4):
                values = tok[q, rows, :].astype(F32) + code(high if q < 2 else low, q % 2)
                values = jnp.where(real > 0.5, values, 0.0)
                gv[q, 0] = values[:, 0:HALF]
                gv[q, 1] = values[:, HALF:]
                centre = centre + jnp.sum(values, axis=1, keepdims=True)
            centre = centre * (1.0 / D)
            square = jnp.zeros((ROWS, 1), F32)
            for q in range(4):
                for h in range(2):
                    shifted = gv[q, h] - centre
                    square = square + jnp.sum(shifted * shifted, axis=1, keepdims=True)
            scale = lax.rsqrt(square * (1.0 / D) + norm_eps)
            place(k, zh, [gv[2 * b + i // 2, i % 2] for i in range(4)], centre, scale)
            valid[k, zh] = real
            cols = jnp.zeros((ROWS, 128), F32)
            for i, value in enumerate((centre, scale, high, low, real)):
                cols = jnp.where(lane == i, value, cols)
            meta_s[k] = cols.T[0:8, :]

    def meta_copy():
        return remote(meta_s, meta_r, ts_s.at[2], ts_r.at[2], y_peer)

    def share_copy(i):
        ref = oth.at[c, pl.ds(256 * i, 256)]
        return remote(ref, ref, ts_s.at[3 + i], ts_r.at[3 + i], core_peer)

    def embed_other(k):
        with jax.named_scope("embed_other"):
            rows = slice(ROWS * k, ROWS * (k + 1))
            cols = jnp.concatenate([meta_r[k]] * 16, axis=0).T
            centre, scale, high, low, real = [cols[:, i : i + 1] for i in range(5)]
            index = jnp.where(b == 0, high, low)
            blocks = []
            for q in range(2):
                values = oth[q, rows, :].astype(F32) + code(index, q)
                values = jnp.where(real > 0.5, values, 0.0)
                blocks += [values[:, 0:HALF], values[:, HALF:]]
            place(k, 1 - zh, blocks, centre, scale)
            valid[k, 1 - zh] = real

    def share(i):
        with jax.named_scope("token_wait"):
            token_copy(i).wait_recv()
        share_copy(i).start()

    def share(i):
        with jax.named_scope("token_wait"):
            token_copy(i).wait_recv()
        share_copy(i).start()

    def y_copy(k):
        return remote(ysend.at[k], yrecv.at[k], y_s.at[k], y_r.at[k], y_peer)

    def core_copy(s):
        ref = xbuf.at[(s // 4 + 1) % 2, s % 4, mine]
        return remote(ref, ref, xd_s.at[s % 8], xd_r.at[s % 8], core_peer)

    def chip_copy(s):
        ref = xbuf.at[(s // 4 + 1) % 2, s % 4, mine]
        return remote(ref, ref, xi_s.at[s % 8], xi_r.at[s % 8], x_peer)

    def pass_copy(s):
        ref = xbuf.at[(s // 4 + 1) % 2, s % 4, block_of(2)]
        return remote(ref, ref, f_s.at[s % 8], f_r.at[s % 8], core_peer)

    def stat_copies(s):
        return [
            remote(
                statbuf.at[s, 0], statbuf.at[s, r], st_s.at[s % 8], st_r.at[s % 8], column(r)
            )
            for r in range(1, 8)
        ]

    def final_place(k):
        return mixed_out.at[pl.ds(k * ROWS, ROWS), pl.ds(pl.multiple_of(c * HALF, HALF), HALF)]

    def final_copy(k):
        return remote(
            xbuf.at[0, k, 0, a], final_place(k), fin_s.at[k, 0], fin_r.at[k, c],
            at(x, y, zh, 1 - zl, a),
        )

    def final_core(k):
        return remote(
            xbuf.at[0, k, 0, 1 - a], final_place(k), fin_s.at[k, 1], fin_r.at[k, c], core_peer
        )

    def final_recv(k, part):
        dst = mixed_out.at[pl.ds(k * ROWS, ROWS), pl.ds(part * HALF, HALF)]
        return pltpu.make_async_copy(xbuf.at[0, k, 0, 0], dst, fin_r.at[k, part])

    def normalise(s):
        with jax.named_scope("normalise"):
            last = s - 4
            l, k = s // 4, s % 4
            means = [statbuf[last, r, 0:1, :] for r in range(8)]
            mean = means[0]
            for r in range(1, 8):
                mean = mean + means[r]
            mean = mean * 0.125
            spread_sum = jnp.zeros_like(mean)
            for r in range(8):
                off = means[r] - mean
                spread_sum = spread_sum + (statbuf[last, r, 1:2, :] + float(HALF) * off * off)
            scale = lax.rsqrt(spread_sum * (1.0 / D) + norm_eps)
            rows = jnp.concatenate([means[r] - mean for r in range(4)] + [scale] * 4, axis=0)
            cols = jnp.concatenate([rows] * 16, axis=0).T
            scale = cols[:, 4:5]
            for r in range(4):
                i = block_of(r)
                off = cols[:, r : r + 1]
                gain = gain_ref[pl.ds(8 * l + 4 * b + i, 1), :]
                d = xbuf[l % 2, k, i].reshape(2 * ROWS, HALF).astype(F32)
                xbuf[l % 2, k, i] = ((d + off) * scale * gain).astype(BF).reshape(2, ROWS, HALF)

    def product(s, h):
        l, k = s // 4, s % 4
        with jax.named_scope("product"):
            left = jnp.concatenate(
                [xbuf[l % 2, k, i].reshape(2 * ROWS, HALF) for i in range(4)], axis=1
            )

            def column_tile(n, _):
                cols = pl.ds(pl.multiple_of(n * 256, 256), 256)
                right = wb[l, h, :, :, :, cols].reshape(2048, 256)
                tile = jnp.dot(left, right, preferred_element_type=F32)
                acc[:, :, cols] = tile.reshape(2, ROWS, 256)
                return 0

            lax.fori_loop(0, 2, column_tile, 0)

    def last_copy(k, i):
        return remote(ysend.at[k, i], yrecv.at[k, i], yl_s.at[k, i], yl_r.at[k, i], y_peer)

    def give(s):
        k = s % 4
        product(s, 1 - b)

        @pl.when(s < STEPS - 4)
        def _():
            ysend[k] = acc[...].astype(BF)
            y_copy(k).start()

        @pl.when(s >= STEPS - 4)
        def _():
            ysend[k, 0] = acc[1 - b].astype(BF)
            last_copy(k, 0).start()
            gv[k, 0] = acc[b]

    def receive(s):
        k = s % 4
        product(s, b)
        with jax.named_scope("y_wait"):
            y_copy(k).wait_recv()
        with jax.named_scope("receive"):
            values = (stream[k] + acc[...] + yrecv[k].astype(F32)).reshape(2 * ROWS, HALF)
            stream[k] = values.reshape(2, ROWS, HALF)
            mean = jnp.sum(values, axis=1, keepdims=True) * (1.0 / HALF)
            d = values - mean
            square = jnp.sum(d * d, axis=1, keepdims=True)
            lanes = lax.broadcasted_iota(jnp.int32, (2 * ROWS, 128), 1)
            cols = jnp.where(lanes == 0, mean, jnp.where(lanes == 1, square, 0.0))
            statbuf[s, 0] = cols.T[0:2, :]
            xbuf[(s // 4 + 1) % 2, k, mine] = d.astype(BF).reshape(2, ROWS, HALF)
            start_all(stat_copies(s))
            chip_copy(s).start()
            core_copy(s).start()

    def give_rest(s):
        k = s % 4
        product(s, b)
        ysend[k, 1] = (acc[1 - b] + stream[k, 1 - b]).astype(BF)
        last_copy(k, 1).start()
        gv[k, 1] = acc[b] + stream[k, b]

    def finish(s, i):
        k = s % 4
        with jax.named_scope("y_wait"):
            last_copy(k, 1 - i).wait_recv()
        with jax.named_scope("finish"):
            real = valid[k, zh] > 0.5
            values = gv[k, i] + yrecv[k, 1 - i].astype(F32)
            xbuf[0, k, 0, i] = jnp.where(real, values, 0.0).astype(BF)

    def finish_both(s):
        k = s % 4
        finish(s, a)
        final_copy(k).start()
        finish(s, 1 - a)

        @pl.when(c == a)
        def _():
            dst = final_place(k)
            pltpu.make_async_copy(xbuf.at[0, k, 0, 1 - a], dst, fin_r.at[k, c]).start()

        @pl.when(c != a)
        def _():
            final_core(k).start()

    def body(s, _):
        @pl.when((s >= 4) & (s < STEPS))
        def _():
            with jax.named_scope("chip_wait"):
                chip_copy(s - 4).wait_recv()
            pass_copy(s - 4).start()

        @pl.when(s < STEPS - 2)
        def _():
            @pl.when(s % 4 == 2)
            def _():
                plane_done((s - 2) // 2 + 1)

            receive(s - 2)

        @pl.when((s == STEPS - 3) | (s == STEPS - 2))
        def _():
            @pl.when(s == STEPS - 3)
            def _():
                plane_done(2 * LAYERS - 1)

            give_rest(s - 1)

        @pl.when(s >= STEPS - 1)
        def _():
            finish_both(s - 3)

        @pl.when((s >= 4) & (s < STEPS))
        def _():
            last = s - 4
            with jax.named_scope("stat_wait"):
                y_copy(s % 4).wait_send()
                seven = statbuf.at[last, pl.ds(1, 7)]
                pltpu.make_async_copy(seven, seven, st_s.at[last % 8]).wait()
                pltpu.make_async_copy(seven, seven, st_r.at[last % 8]).wait()
            with jax.named_scope("block_wait"):
                core_copy(last).wait()
                chip_copy(last).wait_send()
                pass_copy(last).wait()
            normalise(s)

            @pl.when(s % 4 == 0)
            def _():
                plane_done(s // 2)

            late = s >= STEPS - 2

            @pl.when(late & (a == 0))
            def _():
                give_rest(s)

            give(s)

            @pl.when(late & (a == 1))
            def _():
                give_rest(s)

        @pl.when((s % 2 == 0) & (s < STEPS - 2))
        def _():
            q = s // 2 + 1

            @pl.when(q + 1 < 2 * LAYERS)
            def _():
                own_on(q + 1)

            line_on(q)

            @pl.when(q + 2 < 2 * LAYERS)
            def _():
                own_out(q + 2)

        @pl.when((s % 2 == 1) & (s < STEPS - 3))
        def _():
            line_out((s + 3) // 2)

        return 0

    weights_kept()
    own_out(0)
    embed_own(0)
    own_on(0)
    own_out(1)
    embed_own(1)
    line_out(0)
    embed_own(2)
    own_on(1)
    embed_own(3)
    meta_copy().start()
    start_outputs()
    line_on(0)
    share(0)
    with jax.named_scope("meta_wait"):
        meta_copy().wait_recv()
        share_copy(0).wait_recv()
    embed_other(0)
    own_out(2)
    line_out(1)
    share(1)
    plane_done(0)
    weights_sent()
    give(0)
    own_on(2)
    embed_other(1)
    give(1)
    line_on(1)
    own_out(3)
    with jax.named_scope("share_wait"):
        share_copy(1).wait_recv()
    embed_other(2)
    give(2)
    embed_other(3)
    line_out(2)
    plane_done(1)
    receive(0)
    give(3)
    own_on(3)
    line_on(2)
    own_out(4)
    lax.fori_loop(3, STEPS + 3, body, 0)

    for k in range(CHUNKS):
        with jax.named_scope("final_wait"):
            for part in (0, 1):
                final_recv(k, part).wait()
        for i in range(2):
            last_copy(k, i).wait_send()
        final_copy(k).wait_send()

        @pl.when(c != a)
        def _(k=k):
            final_core(k).wait_send()

    with jax.named_scope("end_wait"):
        meta_copy().wait_send()
    for i in range(2):
        token_copy(i).wait_send()
        share_copy(i).wait_send()
    def sent(q, _):
        for group in range(4):
            sent_group(q, group)
        return 0

    with jax.named_scope("end_sent"):
        lax.fori_loop(0, 2 * LAYERS, sent, 0)
    for j, dst in enumerate((pv, mv, vv)):
        pltpu.make_async_copy(dst, dst, out_sem.at[j]).wait()


def hand_over(p, m, v, mixed, p_out, m_out, v_out, mixed_out, sem):
    copies = [
        pltpu.make_async_copy(src, dst, sem.at[j])
        for j, (src, dst) in enumerate(((p, p_out), (m, m_out), (v, v_out), (mixed, mixed_out)))
    ]
    for copy in copies:
        copy.start()
    for copy in copies:
        copy.wait()


def per_device(
    tokens, counts, patch_index, clip_limit, norm_gain, params, moments, seconds, gradients
):
    any_space = pl.BlockSpec(memory_space=pl.ANY)
    hbm = pl.BlockSpec(memory_space=pltpu.HBM)
    smem = pl.BlockSpec(memory_space=pltpu.SMEM)
    master = jax.ShapeDtypeStruct((LAYERS, ROWS, 1024), F32)
    dma = pltpu.SemaphoreType.DMA
    shapes = (master, master, master, jax.ShapeDtypeStruct((512, 1024), BF))
    results = pl.pallas_call(
        kernel,
        out_shape=shapes,
        in_specs=[hbm, smem, hbm, smem, hbm] + [hbm] * 4,
        out_specs=(any_space,) * 4,
        scratch_shapes=[
            pltpu.VMEM((LAYERS, ROWS, 1024), F32),
            pltpu.VMEM((LAYERS, ROWS, 1024), F32),
            pltpu.VMEM((LAYERS, ROWS, 1024), F32),
            pltpu.VMEM((LAYERS, 2, ROWS, HALF), F32),
            pltpu.VMEM((LAYERS, 2, 4, 4, ROWS, HALF), BF),
            pltpu.VMEM((4, 512, 1024), BF),
            pltpu.VMEM((2, 512, 1024), BF),
            pltpu.VMEM((2, CHUNKS, 4, 2, ROWS, HALF), BF),
            pltpu.VMEM((CHUNKS, 2, ROWS, HALF), F32),
            pltpu.VMEM((CHUNKS, 2, ROWS, HALF), BF),
            pltpu.VMEM((CHUNKS, 2, ROWS, HALF), BF),
            pltpu.VMEM((2, ROWS, HALF), F32),
            pltpu.VMEM((STEPS - 4, 8, 2, 2 * ROWS), F32),
            pltpu.VMEM((128, 2048), BF),
            pltpu.VMEM((CHUNKS, 2, ROWS, 1), F32),
            pltpu.VMEM((CHUNKS, 8, 128), F32),
            pltpu.VMEM((CHUNKS, 8, 128), F32),
            pltpu.VMEM((2, 16, 8, 128), F32),
            pltpu.VMEM((CHUNKS, 128), jnp.int32),
            pltpu.VMEM((LAYERS, D), F32),
            pltpu.VMEM((32, HALF), F32),
            dma((LAYERS, 2)),
            dma((3,)),
            dma((1,)),
            dma((2,)),
            dma((2,)),
            dma((2,)),
            dma((LAYERS, 2)),
            dma((LAYERS, 2)),
            dma((2 * LAYERS, 4)),
            dma((2 * LAYERS, 4)),
            dma((5,)),
            dma((5,)),
            dma((4,)),
            dma((4,)),
            dma((CHUNKS, 2)),
            dma((CHUNKS, 2)),
            dma((8,)),
            dma((8,)),
            dma((8,)),
            dma((8,)),
            dma((8,)),
            dma((8,)),
            dma((8,)),
            dma((8,)),
            dma((CHUNKS, 2)),
            dma((CHUNKS, 2)),
        ],
        compiler_params=pltpu.CompilerParams(
            collective_id=0, has_side_effects=True, vmem_limit_bytes=49200000
        ),
    )(
        tokens,
        counts,
        pltpu.with_memory_space_constraint(patch_index, pltpu.HBM),
        clip_limit.reshape(1, 1),
        pltpu.with_memory_space_constraint(norm_gain, pltpu.HBM),
        params,
        moments,
        seconds,
        gradients,
    )
    return pl.pallas_call(
        hand_over,
        out_shape=shapes,
        in_specs=[any_space] * 4,
        out_specs=(any_space,) * 4,
        scratch_shapes=[
            dma((4,)),
        ],
        compiler_params=pltpu.CompilerParams(vmem_limit_bytes=1024 * 1024),
    )(*results)


def solution(mesh):
    shard = P(None, "dp", "fsdp")
    return jax.shard_map(
        per_device,
        mesh=mesh,
        in_specs=(P("dp", None), P("dp"), P("dp"), P(), P(), shard, shard, shard, shard),
        out_specs=(shard, shard, shard, P("dp", "fsdp")),
        check_vma=False,
    )
```

```python
import functools
import math

import jax
import jax.numpy as jnp
from jax import lax
from jax.experimental import pallas as pl
from jax.experimental.pallas import tpu as pltpu
from jax.sharding import PartitionSpec as P

D = 4096
LAYERS = 4
STEP = 40
ROWS = 128
HALF = 512
CHUNKS = 4
STEPS = LAYERS * CHUNKS
FIRST = 2 * LAYERS

beta_one = 0.9
beta_two = 0.95
adam_eps = 1e-08
learning_rate = 0.0024
weight_decay = 0.05
norm_eps = 1e-06
BF = jnp.bfloat16
F32 = jnp.float32
MESH = pl.DeviceIdType.MESH


def kernel(
    tokens_hbm, counts_ref, patch_hbm, clip_ref, gain_hbm, params_hbm, moments_hbm, seconds_hbm,
    gradients_hbm, params_out, moments_out, seconds_out, mixed_out,
    pv, mv, vv, gv, wb, tok, oth, xbuf, stream, ysend, yrecv, acc, statbuf,
    table, valid, meta_s, meta_r, red, patch_ref, gain_raw, gain_ref,
    in_sem, out_sem, tok_sem, small_sem, red_s, red_r, wx_s, wx_r, ag_s, ag_r, ts_s, ts_r,
    y_s, y_r, yl_s, yl_r, xd_s, xd_r, xi_s, xi_r, f_s, f_r, st_s, st_r, fin_s, fin_r,
):
    dp = lax.axis_index("dp")
    fs = lax.axis_index("fsdp")
    x = dp % 4
    y = (dp // 4) % 4
    zh = dp // 16
    zl = fs // 2
    c = fs % 2
    b = zh
    a = (zl + zh) % 2
    mine = 2 * a + c

    def flip(v, bit):
        return 1 - v if bit else v

    def at(xx, yy, hh, ll, cc):
        return (hh * 16 + yy * 4 + xx, ll * 2 + cc)

    def along_x(d):
        return at((x + d) % 4, y, zh, zl, c)

    def along_y(d):
        return at(x, (y + d) % 4, zh, zl, c)

    def column(r):
        return at(x, y, flip(zh, r & 4), flip(zl, r & 2), flip(c, r & 1))

    def block_of(r):
        return 2 * flip(a, r & 2) + flip(c, r & 1)

    core_peer = column(1)
    x_peer = column(2)
    y_peer = column(6)

    def remote(src, dst, ssem, rsem, dev):
        return pltpu.make_async_remote_copy(
            src_ref=src, dst_ref=dst, send_sem=ssem, recv_sem=rsem, device_id=dev,
            device_id_type=MESH,
        )

    for l in range(LAYERS):
        for h in range(2):
            pltpu.make_async_copy(
                gradients_hbm.at[l, :, pl.ds(HALF * h, HALF)], gv.at[l, h], in_sem.at[l, 1]
            ).start()
    barrier = pltpu.get_barrier_semaphore()
    plane = [
        at((x + i) % 4, (y + j) % 4, zh, zl, c) for j in range(4) for i in range(4) if i or j
    ]
    others = plane + [column(r) for r in range(1, 8)]
    for dev in others:
        pl.semaphore_signal(barrier, inc=1, device_id=dev, device_id_type=MESH)
    for l in range(LAYERS):
        for src, dst in ((params_hbm, pv), (moments_hbm, mv), (seconds_hbm, vv)):
            pltpu.make_async_copy(src.at[l], dst.at[l], in_sem.at[l, 0]).start()
    for q in range(4):
        pltpu.make_async_copy(
            tokens_hbm.at[:, pl.ds(1024 * q, 1024)], tok.at[q], tok_sem.at[0]
        ).start()
    small = [pltpu.make_async_copy(gain_hbm, gain_raw, small_sem.at[0])]
    for k in range(CHUNKS):
        small.append(
            pltpu.make_async_copy(
                patch_hbm.at[pl.ds(ROWS * k, ROWS)], patch_ref.at[k], small_sem.at[1]
            )
        )
    for copy in small:
        copy.start()

    total = jnp.zeros((8, HALF), F32)
    for l in range(LAYERS):
        pltpu.make_async_copy(gv.at[l], gv.at[l], in_sem.at[l, 1]).wait()

        def squares(i, part, l=l):
            for h in range(2):
                g = gv[l, h, pl.ds(pl.multiple_of(i * 32, 32), 32), :]
                g = g * g
                part = part + ((g[0:8] + g[8:16]) + (g[16:24] + g[24:32]))
            return part

        total = lax.fori_loop(0, 4, squares, total)
    tile = total[:, 0:128]
    for i in range(1, 4):
        tile = tile + total[:, 128 * i : 128 * (i + 1)]
    with jax.named_scope("barrier"):
        pl.semaphore_wait(barrier, len(others))

    def exchange(stage, devs, tile, filler):
        red[stage, 0] = tile
        copies = [
            remote(
                red.at[stage, 0], red.at[stage, r + 1], red_s.at[stage], red_r.at[stage], dev
            )
            for r, dev in enumerate(devs)
        ]
        for copy in copies:
            copy.start()
        filler()
        with jax.named_scope("reduce_wait"):
            came = red.at[stage, pl.ds(1, len(devs))]
            pltpu.make_async_copy(came, came, red_s.at[stage]).wait()
            pltpu.make_async_copy(came, came, red_r.at[stage]).wait()
            for r in range(len(devs)):
                tile = tile + red[stage, r + 1]
        return tile

    def token_copy(i):
        rows = pl.ds(256 * i, 256)
        return remote(
            tok.at[2 * (1 - b) + c, rows], oth.at[c, rows], ts_s.at[i], ts_r.at[i], y_peer
        )

    def fill_column():
        pltpu.make_async_copy(tok, tok, tok_sem.at[0]).wait()
        token_copy(0).start()
        token_copy(1).start()

    def fill_table():
        lane = lax.broadcasted_iota(jnp.int32, (16, 1024), 1).astype(F32)
        row = lax.broadcasted_iota(jnp.int32, (16, 1024), 0).astype(F32)
        angle = row * jnp.exp(lane * (-math.log(10000.0) / 1024.0))
        for q, wave in ((0, jnp.sin(angle)), (1, jnp.cos(angle))):
            cols = slice(1024 * q, 1024 * (q + 1))
            for i in range(3):
                piece = wave.astype(BF)
                table[16 * i : 16 * (i + 1), cols] = piece
                wave = wave - piece.astype(F32)
        table[48:128, :] = jnp.zeros((80, 2048), BF)
        small[0].wait()
        pltpu.make_async_copy(patch_ref, patch_ref, small_sem.at[1]).wait()
        for l in range(LAYERS):
            for i in range(8):
                gain_ref[8 * l + i : 8 * l + i + 1, :] = gain_raw[
                    l : l + 1, HALF * i : HALF * (i + 1)
                ]

    tile = exchange(0, [column(r) for r in range(1, 8)], tile, fill_column)
    tile = exchange(1, plane, tile, fill_table)
    norm = jnp.sqrt(jnp.sum(jnp.sum(tile, axis=1, keepdims=True), axis=0, keepdims=True))
    factor = jnp.minimum(1.0, clip_ref[0, 0] / (norm + 1e-06))

    def weight_copies(l):
        here = wb.at[l, zl, y, x]
        keep = pltpu.make_async_copy(ysend.at[l, c], here, wx_s.at[1])
        give = remote(ysend.at[l, 1 - c], here, wx_s.at[0], wx_r.at[l, 0], core_peer)
        same = remote(ysend.at[l, c], here, wx_s.at[0], wx_r.at[l, 1], x_peer)
        cross = remote(ysend.at[l, 1 - c], here, wx_s.at[1], wx_r.at[l, 1], column(3))
        return keep, give, same, cross

    for l in range(LAYERS):
        three = pv.at[pl.ds(0, 3)]
        pltpu.make_async_copy(three, three, in_sem.at[l, 0]).wait()

        def update(i, _, l=l):
            rows = pl.ds(pl.multiple_of(i * 16, 16), 16)
            p = pv[l, rows, :]
            clipped = jnp.concatenate([gv[l, 0, rows, :], gv[l, 1, rows, :]], axis=1) * factor
            m = beta_one * mv[l, rows, :] + (1.0 - beta_one) * clipped
            v = beta_two * vv[l, rows, :] + (1.0 - beta_two) * clipped * clipped
            root = jnp.sqrt(v * (1.0 / (1.0 - beta_two**STEP))) + adam_eps
            direction = (m * (1.0 / (1.0 - beta_one**STEP))) / root
            p = p - learning_rate * (direction + weight_decay * p)
            mv[l, rows, :] = m
            vv[l, rows, :] = v
            pv[l, rows, :] = p
            w = p.astype(BF)
            ysend[l, 0, rows, :] = w[:, 0:HALF]
            ysend[l, 1, rows, :] = w[:, HALF:]
            return 0

        with jax.named_scope("update"):
            lax.fori_loop(0, ROWS // 16, update, 0)
        own, give_core, same, cross = weight_copies(l)

        @pl.when(c == a)
        def _():
            own.start()
            give_core.start()

        @pl.when(c != a)
        def _():
            same.start()
            cross.start()

    def four_blocks(sem):
        ref = ysend.at[pl.ds(0, 2)]
        pltpu.make_async_copy(ref, ref, sem).wait()

    def weights_kept():
        @pl.when(c == a)
        def _():
            four_blocks(wx_s.at[1])

    def weights_sent():
        four_blocks(wx_s.at[0])

        @pl.when(c != a)
        def _():
            four_blocks(wx_s.at[1])

    def start_outputs():
        for l in range(LAYERS):
            for j, (src, dst) in enumerate(((pv, params_out), (mv, moments_out), (vv, seconds_out))):
                pltpu.make_async_copy(src.at[l], dst.at[l], out_sem.at[j]).start()

    def piece(q, h, phase, xx, yy, part):
        if isinstance(q, int) and q in (0, FIRST):
            cols = pl.ds(256 * (q // FIRST), 256)
            if phase == 0:
                return wb.at[0, 1 - b, yy, xx, pl.ds(64 * h + 32 * part, 32), cols]
            if h == 0:
                return wb.at[0, 1 - b, yy, pl.ds(2 * part, 2), pl.ds(0, 64), cols]
            return wb.at[0, 1 - b, pl.ds(2 * part, 2), xx, pl.ds(64, 64), cols]
        l, nb = q // 2, (1 - b) + (q % 2) * (2 * b - 1)
        if phase == 0:
            return wb.at[l, nb, yy, xx, pl.ds(64 * h + 32 * part, 32), :]
        if h == 0:
            return wb.at[l, nb, yy, pl.ds(2 * part, 2), pl.ds(0, 64), :]
        return wb.at[l, nb, pl.ds(2 * part, 2), xx, pl.ds(64, 64), :]

    def gather_copy(q, h, phase, sign, kind):
        on_x = (h == 0) == (phase == 0)
        step = 1 if sign == 0 else 3
        part = sign if kind != 1 else 1 - sign
        xx, yy = x, y
        if kind == 2:
            if on_x:
                xx = (x + 4 - step) % 4
            else:
                yy = (y + 4 - step) % 4
        ref = piece(q, h, phase, xx, yy, part)
        group = 2 * phase + (0 if kind == 0 else 1)
        layer = 0 if isinstance(q, int) and q == FIRST else q // 2
        out = layer if phase == 1 else LAYERS
        dev = along_x(step) if on_x else along_y(step)
        return remote(ref, ref, ag_s.at[out], ag_r.at[q, group], dev)

    def both(q, phase, kind):
        return [gather_copy(q, h, phase, sign, kind) for h in (0, 1) for sign in (0, 1)]

    def start_all(copies):
        for copy in copies:
            copy.start()

    def group_ref(q, group):
        if isinstance(q, int) and q in (0, FIRST):
            if group == 0:
                return wb.at[0, 0, 0, 0, pl.ds(0, 64)]
            return wb.at[0, 0, 0, pl.ds(0, 2 ** (group - 1))]
        l, nb = q // 2, q % 2
        if group < 2:
            return wb.at[l, nb, 0, pl.ds(0, group + 1)]
        return wb.at[l, nb, pl.ds(0, group - 1)]

    def recv_group(q, group):
        ref = group_ref(q, group)
        pltpu.make_async_copy(ref, ref, ag_r.at[q, group]).wait()

    def own_out(q):
        with jax.named_scope("own_out"):
            if not (isinstance(q, int) and q == FIRST):
                l, nb = q // 2, (1 - b) + (q % 2) * (2 * b - 1)
                here = wb.at[l, nb, y, x]

                @pl.when((c != a) | (nb != zl))
                def _():
                    pltpu.make_async_copy(here, here, wx_r.at[l, (nb + zl) % 2]).wait()

            start_all(both(q, 0, 0))
            start_all(both(q, 0, 1))

    def own_on(q):
        with jax.named_scope("own_on"):
            recv_group(q, 0)
            start_all(both(q, 0, 2))

    def line_out(q):
        with jax.named_scope("line_out"):
            recv_group(q, 1)
            start_all(both(q, 1, 0))
            if isinstance(q, int) and q == FIRST:
                return
            start_all(both(q, 1, 1))

    def line_on(q):
        with jax.named_scope("line_on"):
            recv_group(q, 2)
            start_all(both(q, 1, 2))

    def plane_done(q):
        with jax.named_scope("plane_done"):
            recv_group(q, 3)

    lane = lax.broadcasted_iota(jnp.int32, (ROWS, 128), 1)
    lane_f = lane.astype(F32)

    def spread(index):
        hit = (lane_f == index) | (lane_f == index + 16.0) | (lane_f == index + 32.0)
        return jnp.where(hit, 1.0, 0.0).astype(BF)

    def code(index, q):
        return jnp.dot(
            spread(index), table[:, 1024 * q : 1024 * (q + 1)], preferred_element_type=F32
        )

    def place(k, side, blocks, centre, scale):
        for q in range(2):
            for h in range(2):
                i = 2 * q + h
                values = blocks[i]
                gain = gain_ref[pl.ds(4 * b + i, 1), :]
                xbuf[0, k, i, side] = ((values - centre) * scale * gain).astype(BF)

                @pl.when(mine == i)
                def _(values=values):
                    stream[k, side] = values

    def embed_own(k):
        with jax.named_scope("embed_own"):
            rows = slice(ROWS * k, ROWS * (k + 1))
            p = jnp.broadcast_to(patch_ref[k : k + 1, :], (ROWS, 128)).T[:, 0:1]
            high = (p // 16).astype(F32)
            low = (p % 16).astype(F32)
            slot = lax.broadcasted_iota(jnp.int32, (ROWS, 1), 0) + ROWS * k
            real = jnp.where(slot < counts_ref[0], 1.0, 0.0)
            centre = jnp.zeros((ROWS, 1), F32)
            for q in range(4):
                values = tok[q, rows, :].astype(F32) + code(high if q < 2 else low, q % 2)
                values = jnp.where(real > 0.5, values, 0.0)
                gv[q, 0] = values[:, 0:HALF]
                gv[q, 1] = values[:, HALF:]
                centre = centre + jnp.sum(values, axis=1, keepdims=True)
            centre = centre * (1.0 / D)
            square = jnp.zeros((ROWS, 1), F32)
            for q in range(4):
                for h in range(2):
                    shifted = gv[q, h] - centre
                    square = square + jnp.sum(shifted * shifted, axis=1, keepdims=True)
            scale = lax.rsqrt(square * (1.0 / D) + norm_eps)
            place(k, zh, [gv[2 * b + i // 2, i % 2] for i in range(4)], centre, scale)
            valid[k, zh] = real
            cols = jnp.zeros((ROWS, 128), F32)
            for i, value in enumerate((centre, scale, high, low, real)):
                cols = jnp.where(lane == i, value, cols)
            meta_s[k] = cols.T[0:8, :]

    def meta_copy():
        return remote(meta_s, meta_r, ts_s.at[2], ts_r.at[2], y_peer)

    def share_copy(i):
        ref = oth.at[c, pl.ds(256 * i, 256)]
        return remote(ref, ref, ts_s.at[3 + i], ts_r.at[3 + i], core_peer)

    def embed_other(k):
        with jax.named_scope("embed_other"):
            rows = slice(ROWS * k, ROWS * (k + 1))
            cols = jnp.concatenate([meta_r[k]] * 16, axis=0).T
            centre, scale, high, low, real = [cols[:, i : i + 1] for i in range(5)]
            index = jnp.where(b == 0, high, low)
            blocks = []
            for q in range(2):
                values = oth[q, rows, :].astype(F32) + code(index, q)
                values = jnp.where(real > 0.5, values, 0.0)
                blocks += [values[:, 0:HALF], values[:, HALF:]]
            place(k, 1 - zh, blocks, centre, scale)
            valid[k, 1 - zh] = real

    def share(i):
        with jax.named_scope("token_wait"):
            token_copy(i).wait_recv()
        share_copy(i).start()

    def share(i):
        with jax.named_scope("token_wait"):
            token_copy(i).wait_recv()
        share_copy(i).start()

    def y_copy(k):
        return remote(ysend.at[k], yrecv.at[k], y_s.at[k], y_r.at[k], y_peer)

    def core_copy(s):
        ref = xbuf.at[(s // 4 + 1) % 2, s % 4, mine]
        return remote(ref, ref, xd_s.at[s % 4], xd_r.at[s % 8], core_peer)

    def chip_copy(s):
        ref = xbuf.at[(s // 4 + 1) % 2, s % 4, mine]
        return remote(ref, ref, xi_s.at[s % 4], xi_r.at[s % 8], x_peer)

    def pass_copy(s):
        ref = xbuf.at[(s // 4 + 1) % 2, s % 4, block_of(2)]
        return remote(ref, ref, f_s.at[s % 4], f_r.at[s % 8], core_peer)

    def stat_copies(s):
        return [
            remote(
                statbuf.at[s, 0], statbuf.at[s, r], st_s.at[s % 4], st_r.at[s % 8], column(r)
            )
            for r in range(1, 8)
        ]

    def final_place(k):
        return mixed_out.at[pl.ds(k * ROWS, ROWS), pl.ds(pl.multiple_of(c * HALF, HALF), HALF)]

    def final_copy(k):
        return remote(
            xbuf.at[0, k, 0, a], final_place(k), fin_s.at[0], fin_r.at[0],
            at(x, y, zh, 1 - zl, a),
        )

    def final_core(k):
        return remote(
            xbuf.at[0, k, 0, 1 - a], final_place(k), fin_s.at[1], fin_r.at[0], core_peer
        )

    def normalise(s):
        with jax.named_scope("normalise"):
            last = s - 4
            l, k = s // 4, s % 4
            means = [statbuf[last, r, 0:1, :] for r in range(8)]
            mean = means[0]
            for r in range(1, 8):
                mean = mean + means[r]
            mean = mean * 0.125
            spread_sum = jnp.zeros_like(mean)
            for r in range(8):
                off = means[r] - mean
                spread_sum = spread_sum + (statbuf[last, r, 1:2, :] + float(HALF) * off * off)
            scale = lax.rsqrt(spread_sum * (1.0 / D) + norm_eps)
            rows = jnp.concatenate([means[r] - mean for r in range(4)] + [scale] * 4, axis=0)
            cols = jnp.concatenate([rows] * 16, axis=0).T
            scale = cols[:, 4:5]
            for r in range(4):
                i = block_of(r)
                off = cols[:, r : r + 1]
                gain = gain_ref[pl.ds(8 * l + 4 * b + i, 1), :]
                d = xbuf[l % 2, k, i].reshape(2 * ROWS, HALF).astype(F32)
                xbuf[l % 2, k, i] = ((d + off) * scale * gain).astype(BF).reshape(2, ROWS, HALF)

    def product(s, h, first=0, tiles=2):
        l, k = s // 4, s % 4
        with jax.named_scope("product"):
            left = jnp.concatenate(
                [xbuf[l % 2, k, i].reshape(2 * ROWS, HALF) for i in range(4)], axis=1
            )

            def column_tile(n, _):
                cols = pl.ds(pl.multiple_of(n * 256, 256), 256)
                right = wb[l, h, :, :, :, cols].reshape(2048, 256)
                tile = jnp.dot(left, right, preferred_element_type=F32)
                acc[:, :, cols] = tile.reshape(2, ROWS, 256)
                return 0

            lax.fori_loop(first, first + tiles, column_tile, 0)

    def part_copy(k, i):
        ref = yrecv.at[k, :, :, pl.ds(256 * i, 256)]
        return remote(
            ysend.at[k, :, :, pl.ds(256 * i, 256)], ref, yl_s.at[k, i], yl_r.at[k, i], y_peer
        )

    def give_first(k, i):
        product(k, 1 - b, i, 1)
        cols = slice(256 * i, 256 * (i + 1))
        ysend[k, :, :, cols] = acc[:, :, cols].astype(BF)
        part_copy(k, i).start()

    def received(s):
        k = s % 4

        @pl.when(s < 4)
        def _():
            part_copy(k, 0).wait_recv()
            part_copy(k, 1).wait_recv()

        @pl.when(s >= 4)
        def _():
            y_copy(k).wait_recv()

    def sent_before(s):
        k = s % 4

        @pl.when(s < 8)
        def _():
            part_copy(k, 0).wait_send()
            part_copy(k, 1).wait_send()

        @pl.when(s >= 8)
        def _():
            y_copy(k).wait_send()

    def last_copy(k, i):
        return remote(ysend.at[k, i], yrecv.at[k, i], yl_s.at[k, i], yl_r.at[k, i], y_peer)

    def give(s):
        k = s % 4
        product(s, 1 - b)

        @pl.when(s < STEPS - 4)
        def _():
            ysend[k] = acc[...].astype(BF)
            y_copy(k).start()

        @pl.when(s >= STEPS - 4)
        def _():
            ysend[k, 0] = acc[1 - b].astype(BF)
            last_copy(k, 0).start()
            gv[k, 0] = acc[b]

    def receive(s):
        k = s % 4
        product(s, b)
        with jax.named_scope("y_wait"):
            received(s)
        with jax.named_scope("receive"):
            values = (stream[k] + acc[...] + yrecv[k].astype(F32)).reshape(2 * ROWS, HALF)
            stream[k] = values.reshape(2, ROWS, HALF)
            mean = jnp.sum(values, axis=1, keepdims=True) * (1.0 / HALF)
            d = values - mean
            square = jnp.sum(d * d, axis=1, keepdims=True)
            lanes = lax.broadcasted_iota(jnp.int32, (2 * ROWS, 128), 1)
            cols = jnp.where(lanes == 0, mean, jnp.where(lanes == 1, square, 0.0))
            statbuf[s, 0] = cols.T[0:2, :]
            xbuf[(s // 4 + 1) % 2, k, mine] = d.astype(BF).reshape(2, ROWS, HALF)
            start_all(stat_copies(s))
            chip_copy(s).start()
            core_copy(s).start()

    def give_rest(s):
        k = s % 4
        product(s, b)
        ysend[k, 1] = (acc[1 - b] + stream[k, 1 - b]).astype(BF)
        last_copy(k, 1).start()
        gv[k, 1] = acc[b] + stream[k, b]

    def finish(s, i):
        k = s % 4
        with jax.named_scope("y_wait"):
            last_copy(k, 1 - i).wait_recv()
        with jax.named_scope("finish"):
            real = valid[k, zh] > 0.5
            values = gv[k, i] + yrecv[k, 1 - i].astype(F32)
            xbuf[0, k, 0, i] = jnp.where(real, values, 0.0).astype(BF)

    def finish_both(s):
        k = s % 4
        finish(s, a)
        final_copy(k).start()
        finish(s, 1 - a)

        @pl.when(c == a)
        def _():
            dst = final_place(k)
            pltpu.make_async_copy(xbuf.at[0, k, 0, 1 - a], dst, fin_r.at[0]).start()

        @pl.when(c != a)
        def _():
            final_core(k).start()

    def body(s, _):
        @pl.when((s >= 4) & (s < STEPS))
        def _():
            with jax.named_scope("chip_wait"):
                chip_copy(s - 4).wait_recv()
            pass_copy(s - 4).start()

        @pl.when(s < STEPS - 2)
        def _():
            @pl.when(s % 4 == 2)
            def _():
                plane_done((s - 2) // 2 + 1)

            receive(s - 2)

        @pl.when((s == STEPS - 3) | (s == STEPS - 2))
        def _():
            @pl.when(s == STEPS - 3)
            def _():
                plane_done(2 * LAYERS - 1)

            give_rest(s - 1)

        @pl.when(s >= STEPS - 1)
        def _():
            finish_both(s - 3)

        @pl.when((s >= 4) & (s < STEPS))
        def _():
            last = s - 4
            with jax.named_scope("stat_wait"):
                sent_before(s)
                seven = statbuf.at[last, pl.ds(1, 7)]
                pltpu.make_async_copy(seven, seven, st_s.at[last % 4]).wait()
                pltpu.make_async_copy(seven, seven, st_r.at[last % 8]).wait()
            with jax.named_scope("block_wait"):
                core_copy(last).wait()
                chip_copy(last).wait_send()
                pass_copy(last).wait()
            normalise(s)

            @pl.when(s % 4 == 0)
            def _():
                plane_done(s // 2)

            late = s >= STEPS - 2

            @pl.when(late & (a == 0))
            def _():
                give_rest(s)

            give(s)

            @pl.when(late & (a == 1))
            def _():
                give_rest(s)

        @pl.when((s % 2 == 0) & (s < STEPS - 2))
        def _():
            q = s // 2 + 1

            @pl.when(q + 1 < 2 * LAYERS)
            def _():
                own_on(q + 1)

            line_on(q)

            @pl.when(q + 2 < 2 * LAYERS)
            def _():
                own_out(q + 2)

        @pl.when((s % 2 == 1) & (s < STEPS - 3))
        def _():
            line_out((s + 3) // 2)

        return 0

    weights_kept()
    own_out(0)
    own_out(FIRST)
    embed_own(0)
    own_on(0)
    own_on(FIRST)
    own_out(1)
    embed_own(1)
    line_out(0)
    line_out(FIRST)
    embed_own(2)
    own_on(1)
    embed_own(3)
    meta_copy().start()
    start_outputs()
    line_on(0)
    start_all(both(FIRST, 1, 1))
    share(0)
    with jax.named_scope("meta_wait"):
        meta_copy().wait_recv()
        share_copy(0).wait_recv()
    line_on(FIRST)
    own_out(2)
    embed_other(0)
    weights_sent()
    plane_done(0)
    give_first(0, 0)
    line_out(1)
    share(1)
    embed_other(1)
    give_first(1, 0)
    own_on(2)
    plane_done(FIRST)
    give_first(0, 1)
    give_first(1, 1)
    line_on(1)
    own_out(3)
    with jax.named_scope("share_wait"):
        share_copy(1).wait_recv()
    embed_other(2)
    give_first(2, 0)
    give_first(2, 1)
    embed_other(3)
    line_out(2)
    plane_done(1)
    receive(0)
    give_first(3, 0)
    give_first(3, 1)
    own_on(3)
    line_on(2)
    own_out(4)
    lax.fori_loop(3, STEPS + 3, body, 0)

    with jax.named_scope("final_wait"):
        pltpu.make_async_copy(mixed_out, mixed_out, fin_r.at[0]).wait()
    four_blocks(fin_s.at[0])

    @pl.when(c != a)
    def _():
        four_blocks(fin_s.at[1])

    for k in range(CHUNKS):
        for i in range(2):
            last_copy(k, i).wait_send()
    with jax.named_scope("end_wait"):
        meta_copy().wait_send()
    for i in range(2):
        token_copy(i).wait_send()
        share_copy(i).wait_send()
    blocks = wb.at[0, :, pl.ds(0, 3)]
    for i in range(LAYERS + 1):
        pltpu.make_async_copy(blocks, blocks, ag_s.at[i]).wait()
    for j, dst in enumerate((pv, mv, vv)):
        pltpu.make_async_copy(dst, dst, out_sem.at[j]).wait()


def hand_over(p, m, v, mixed, p_out, m_out, v_out, mixed_out, sem):
    copies = [
        pltpu.make_async_copy(src, dst, sem.at[j])
        for j, (src, dst) in enumerate(((p, p_out), (m, m_out), (v, v_out), (mixed, mixed_out)))
    ]
    for copy in copies:
        copy.start()
    for copy in copies:
        copy.wait()


def per_device(
    tokens, counts, patch_index, clip_limit, norm_gain, params, moments, seconds, gradients
):
    any_space = pl.BlockSpec(memory_space=pl.ANY)
    hbm = pl.BlockSpec(memory_space=pltpu.HBM)
    smem = pl.BlockSpec(memory_space=pltpu.SMEM)
    master = jax.ShapeDtypeStruct((LAYERS, ROWS, 1024), F32)
    dma = pltpu.SemaphoreType.DMA
    shapes = (master, master, master, jax.ShapeDtypeStruct((512, 1024), BF))
    results = pl.pallas_call(
        kernel,
        out_shape=shapes,
        in_specs=[hbm, smem, hbm, smem, hbm] + [hbm] * 4,
        out_specs=(any_space,) * 4,
        scratch_shapes=[
            pltpu.VMEM((LAYERS, ROWS, 1024), F32),
            pltpu.VMEM((LAYERS, ROWS, 1024), F32),
            pltpu.VMEM((LAYERS, ROWS, 1024), F32),
            pltpu.VMEM((LAYERS, 2, ROWS, HALF), F32),
            pltpu.VMEM((LAYERS, 2, 4, 4, ROWS, HALF), BF),
            pltpu.VMEM((4, 512, 1024), BF),
            pltpu.VMEM((2, 512, 1024), BF),
            pltpu.VMEM((2, CHUNKS, 4, 2, ROWS, HALF), BF),
            pltpu.VMEM((CHUNKS, 2, ROWS, HALF), F32),
            pltpu.VMEM((CHUNKS, 2, ROWS, HALF), BF),
            pltpu.VMEM((CHUNKS, 2, ROWS, HALF), BF),
            pltpu.VMEM((2, ROWS, HALF), F32),
            pltpu.VMEM((STEPS - 4, 8, 2, 2 * ROWS), F32),
            pltpu.VMEM((128, 2048), BF),
            pltpu.VMEM((CHUNKS, 2, ROWS, 1), F32),
            pltpu.VMEM((CHUNKS, 8, 128), F32),
            pltpu.VMEM((CHUNKS, 8, 128), F32),
            pltpu.VMEM((2, 16, 8, 128), F32),
            pltpu.VMEM((CHUNKS, 128), jnp.int32),
            pltpu.VMEM((LAYERS, D), F32),
            pltpu.VMEM((32, HALF), F32),
            dma((LAYERS, 2)),
            dma((3,)),
            dma((1,)),
            dma((2,)),
            dma((2,)),
            dma((2,)),
            dma((2,)),
            dma((LAYERS, 2)),
            dma((LAYERS + 1,)),
            dma((2 * LAYERS + 1, 4)),
            dma((5,)),
            dma((5,)),
            dma((4,)),
            dma((4,)),
            dma((CHUNKS, 2)),
            dma((CHUNKS, 2)),
            dma((4,)),
            dma((8,)),
            dma((4,)),
            dma((8,)),
            dma((4,)),
            dma((8,)),
            dma((4,)),
            dma((8,)),
            dma((2,)),
            dma((1,)),
        ],
        compiler_params=pltpu.CompilerParams(
            collective_id=0, has_side_effects=True, vmem_limit_bytes=49200000
        ),
    )(
        tokens,
        counts,
        pltpu.with_memory_space_constraint(patch_index, pltpu.HBM),
        clip_limit.reshape(1, 1),
        pltpu.with_memory_space_constraint(norm_gain, pltpu.HBM),
        params,
        moments,
        seconds,
        gradients,
    )
    return pl.pallas_call(
        hand_over,
        out_shape=shapes,
        in_specs=[any_space] * 4,
        out_specs=(any_space,) * 4,
        scratch_shapes=[
            dma((4,)),
        ],
        compiler_params=pltpu.CompilerParams(vmem_limit_bytes=1024 * 1024),
    )(*results)


def solution(mesh):
    shard = P(None, "dp", "fsdp")
    return jax.shard_map(
        per_device,
        mesh=mesh,
        in_specs=(P("dp", None), P("dp"), P("dp"), P(), P(), shard, shard, shard, shard),
        out_specs=(shard, shard, shard, P("dp", "fsdp")),
        check_vma=False,
    )
```

```python
import functools
import math

import jax
import jax.numpy as jnp
from jax import lax
from jax.experimental import pallas as pl
from jax.experimental.pallas import tpu as pltpu
from jax.sharding import PartitionSpec as P

D = 4096
LAYERS = 4
STEP = 40
ROWS = 128
HALF = 512
CHUNKS = 4
STEPS = LAYERS * CHUNKS
FIRST = 2 * LAYERS

beta_one = 0.9
beta_two = 0.95
adam_eps = 1e-08
learning_rate = 0.0024
weight_decay = 0.05
norm_eps = 1e-06
BF = jnp.bfloat16
F32 = jnp.float32
MESH = pl.DeviceIdType.MESH


def kernel(
    tokens_hbm, counts_ref, patch_hbm, clip_ref, gain_hbm, params_hbm, moments_hbm, seconds_hbm,
    gradients_hbm, params_out, moments_out, seconds_out, mixed_out,
    pv, mv, vv, gv, wb, tok, oth, xbuf, stream, ysend, yrecv, acc, statbuf,
    table, valid, meta_s, meta_r, red, patch_ref, gain_raw, gain_ref,
    in_sem, out_sem, tok_sem, small_sem, red_s, red_r, wx_s, wx_r, ag_s, ag_r, ts_s, ts_r,
    y_s, y_r, yl_s, yl_r, xd_s, xd_r, xi_s, xi_r, f_s, f_r, st_s, st_r, fin_s, fin_r,
):
    dp = lax.axis_index("dp")
    fs = lax.axis_index("fsdp")
    x = dp % 4
    y = (dp // 4) % 4
    zh = dp // 16
    zl = fs // 2
    c = fs % 2
    b = zh
    a = (zl + zh) % 2
    mine = 2 * a + c

    def flip(v, bit):
        return 1 - v if bit else v

    def at(xx, yy, hh, ll, cc):
        return (hh * 16 + yy * 4 + xx, ll * 2 + cc)

    def along_x(d):
        return at((x + d) % 4, y, zh, zl, c)

    def along_y(d):
        return at(x, (y + d) % 4, zh, zl, c)

    def column(r):
        return at(x, y, flip(zh, r & 4), flip(zl, r & 2), flip(c, r & 1))

    def block_of(r):
        return 2 * flip(a, r & 2) + flip(c, r & 1)

    core_peer = column(1)
    x_peer = column(2)
    y_peer = column(6)

    def remote(src, dst, ssem, rsem, dev):
        return pltpu.make_async_remote_copy(
            src_ref=src, dst_ref=dst, send_sem=ssem, recv_sem=rsem, device_id=dev,
            device_id_type=MESH,
        )

    for l in range(LAYERS):
        for h in range(2):
            pltpu.make_async_copy(
                gradients_hbm.at[l, :, pl.ds(HALF * h, HALF)], gv.at[l, h], in_sem.at[l, 1]
            ).start()
    barrier = pltpu.get_barrier_semaphore()
    plane = [
        at((x + i) % 4, (y + j) % 4, zh, zl, c) for j in range(4) for i in range(4) if i or j
    ]
    others = plane + [column(r) for r in range(1, 8)]
    for dev in others:
        pl.semaphore_signal(barrier, inc=1, device_id=dev, device_id_type=MESH)
    for l in range(LAYERS):
        for src, dst in ((params_hbm, pv), (moments_hbm, mv), (seconds_hbm, vv)):
            pltpu.make_async_copy(src.at[l], dst.at[l], in_sem.at[l, 0]).start()
    for q in range(4):
        pltpu.make_async_copy(
            tokens_hbm.at[:, pl.ds(1024 * q, 1024)], tok.at[q], tok_sem.at[0]
        ).start()
    small = [pltpu.make_async_copy(gain_hbm, gain_raw, small_sem.at[0])]
    for k in range(CHUNKS):
        small.append(
            pltpu.make_async_copy(
                patch_hbm.at[pl.ds(ROWS * k, ROWS)], patch_ref.at[k], small_sem.at[1]
            )
        )
    for copy in small:
        copy.start()

    total = jnp.zeros((8, HALF), F32)
    for l in range(LAYERS):
        pltpu.make_async_copy(gv.at[l], gv.at[l], in_sem.at[l, 1]).wait()

        def squares(i, part, l=l):
            for h in range(2):
                g = gv[l, h, pl.ds(pl.multiple_of(i * 32, 32), 32), :]
                g = g * g
                part = part + ((g[0:8] + g[8:16]) + (g[16:24] + g[24:32]))
            return part

        total = lax.fori_loop(0, 4, squares, total)
    tile = total[:, 0:128]
    for i in range(1, 4):
        tile = tile + total[:, 128 * i : 128 * (i + 1)]
    with jax.named_scope("barrier"):
        pl.semaphore_wait(barrier, len(others))

    def exchange(stage, devs, tile, filler):
        red[stage, 0] = tile
        copies = [
            remote(
                red.at[stage, 0], red.at[stage, r + 1], red_s.at[stage], red_r.at[stage], dev
            )
            for r, dev in enumerate(devs)
        ]
        for copy in copies:
            copy.start()
        filler()
        with jax.named_scope("reduce_wait"):
            came = red.at[stage, pl.ds(1, len(devs))]
            pltpu.make_async_copy(came, came, red_s.at[stage]).wait()
            pltpu.make_async_copy(came, came, red_r.at[stage]).wait()
            for r in range(len(devs)):
                tile = tile + red[stage, r + 1]
        return tile

    def token_copy(i):
        rows = pl.ds(256 * i, 256)
        return remote(
            tok.at[2 * (1 - b) + c, rows], oth.at[c, rows], ts_s.at[i], ts_r.at[i], y_peer
        )

    def fill_column():
        pltpu.make_async_copy(tok, tok, tok_sem.at[0]).wait()
        token_copy(0).start()
        token_copy(1).start()

    def fill_table():
        lane = lax.broadcasted_iota(jnp.int32, (16, 1024), 1).astype(F32)
        row = lax.broadcasted_iota(jnp.int32, (16, 1024), 0).astype(F32)
        angle = row * jnp.exp(lane * (-math.log(10000.0) / 1024.0))
        for q, wave in ((0, jnp.sin(angle)), (1, jnp.cos(angle))):
            cols = slice(1024 * q, 1024 * (q + 1))
            for i in range(3):
                piece = wave.astype(BF)
                table[16 * i : 16 * (i + 1), cols] = piece
                wave = wave - piece.astype(F32)
        table[48:128, :] = jnp.zeros((80, 2048), BF)
        small[0].wait()
        pltpu.make_async_copy(patch_ref, patch_ref, small_sem.at[1]).wait()
        for l in range(LAYERS):
            for i in range(8):
                gain_ref[8 * l + i : 8 * l + i + 1, :] = gain_raw[
                    l : l + 1, HALF * i : HALF * (i + 1)
                ]

    tile = exchange(0, [column(r) for r in range(1, 8)], tile, fill_column)
    tile = exchange(1, plane, tile, fill_table)
    norm = jnp.sqrt(jnp.sum(jnp.sum(tile, axis=1, keepdims=True), axis=0, keepdims=True))
    factor = jnp.minimum(1.0, clip_ref[0, 0] / (norm + 1e-06))

    def weight_copies(l):
        here = wb.at[l, zl, y, x]
        keep = pltpu.make_async_copy(ysend.at[l, c], here, wx_s.at[1])
        give = remote(ysend.at[l, 1 - c], here, wx_s.at[0], wx_r.at[l, 0], core_peer)
        same = remote(ysend.at[l, c], here, wx_s.at[0], wx_r.at[l, 1], x_peer)
        cross = remote(ysend.at[l, 1 - c], here, wx_s.at[1], wx_r.at[l, 1], column(3))
        return keep, give, same, cross

    for l in range(LAYERS):
        three = pv.at[pl.ds(0, 3)]
        pltpu.make_async_copy(three, three, in_sem.at[l, 0]).wait()

        def update(i, _, l=l):
            rows = pl.ds(pl.multiple_of(i * 16, 16), 16)
            p = pv[l, rows, :]
            clipped = jnp.concatenate([gv[l, 0, rows, :], gv[l, 1, rows, :]], axis=1) * factor
            m = beta_one * mv[l, rows, :] + (1.0 - beta_one) * clipped
            v = beta_two * vv[l, rows, :] + (1.0 - beta_two) * clipped * clipped
            root = jnp.sqrt(v * (1.0 / (1.0 - beta_two**STEP))) + adam_eps
            direction = (m * (1.0 / (1.0 - beta_one**STEP))) / root
            p = p - learning_rate * (direction + weight_decay * p)
            mv[l, rows, :] = m
            vv[l, rows, :] = v
            pv[l, rows, :] = p
            w = p.astype(BF)
            ysend[l, 0, rows, :] = w[:, 0:HALF]
            ysend[l, 1, rows, :] = w[:, HALF:]
            return 0

        with jax.named_scope("update"):
            lax.fori_loop(0, ROWS // 16, update, 0)
        own, give_core, same, cross = weight_copies(l)

        @pl.when(c == a)
        def _():
            own.start()
            give_core.start()

        @pl.when(c != a)
        def _():
            same.start()
            cross.start()

    def four_blocks(sem):
        ref = ysend.at[pl.ds(0, 2)]
        pltpu.make_async_copy(ref, ref, sem).wait()

    def weights_kept():
        @pl.when(c == a)
        def _():
            four_blocks(wx_s.at[1])

    def weights_sent():
        four_blocks(wx_s.at[0])

        @pl.when(c != a)
        def _():
            four_blocks(wx_s.at[1])

    def start_outputs():
        for l in range(LAYERS):
            for j, (src, dst) in enumerate(((pv, params_out), (mv, moments_out), (vv, seconds_out))):
                pltpu.make_async_copy(src.at[l], dst.at[l], out_sem.at[j]).start()

    def piece(q, h, phase, xx, yy, part):
        if isinstance(q, int) and q in (0, FIRST):
            cols = pl.ds(256 * (q // FIRST), 256)
            if phase == 0:
                return wb.at[0, 1 - b, yy, xx, pl.ds(64 * h + 32 * part, 32), cols]
            if h == 0:
                return wb.at[0, 1 - b, yy, pl.ds(2 * part, 2), pl.ds(0, 64), cols]
            return wb.at[0, 1 - b, pl.ds(2 * part, 2), xx, pl.ds(64, 64), cols]
        l, nb = q // 2, (1 - b) + (q % 2) * (2 * b - 1)
        if phase == 0:
            return wb.at[l, nb, yy, xx, pl.ds(64 * h + 32 * part, 32), :]
        if h == 0:
            return wb.at[l, nb, yy, pl.ds(2 * part, 2), pl.ds(0, 64), :]
        return wb.at[l, nb, pl.ds(2 * part, 2), xx, pl.ds(64, 64), :]

    def gather_copy(q, h, phase, sign, kind):
        on_x = (h == 0) == (phase == 0)
        step = 1 if sign == 0 else 3
        part = sign if kind != 1 else 1 - sign
        xx, yy = x, y
        if kind == 2:
            if on_x:
                xx = (x + 4 - step) % 4
            else:
                yy = (y + 4 - step) % 4
        ref = piece(q, h, phase, xx, yy, part)
        group = 2 * phase + (0 if kind == 0 else 1)
        layer = 0 if isinstance(q, int) and q == FIRST else q // 2
        out = layer if phase == 1 else LAYERS
        dev = along_x(step) if on_x else along_y(step)
        return remote(ref, ref, ag_s.at[out], ag_r.at[q, group], dev)

    def both(q, phase, kind):
        return [gather_copy(q, h, phase, sign, kind) for h in (0, 1) for sign in (0, 1)]

    def start_all(copies):
        for copy in copies:
            copy.start()

    def group_ref(q, group):
        if isinstance(q, int) and q in (0, FIRST):
            if group == 0:
                return wb.at[0, 0, 0, 0, pl.ds(0, 64)]
            return wb.at[0, 0, 0, pl.ds(0, 2 ** (group - 1))]
        l, nb = q // 2, q % 2
        if group < 2:
            return wb.at[l, nb, 0, pl.ds(0, group + 1)]
        return wb.at[l, nb, pl.ds(0, group - 1)]

    def recv_group(q, group):
        ref = group_ref(q, group)
        pltpu.make_async_copy(ref, ref, ag_r.at[q, group]).wait()

    def own_out(q):
        with jax.named_scope("own_out"):
            if not (isinstance(q, int) and q == FIRST):
                l, nb = q // 2, (1 - b) + (q % 2) * (2 * b - 1)
                here = wb.at[l, nb, y, x]

                @pl.when((c != a) | (nb != zl))
                def _():
                    pltpu.make_async_copy(here, here, wx_r.at[l, (nb + zl) % 2]).wait()

            start_all(both(q, 0, 0))
            start_all(both(q, 0, 1))

    def own_on(q):
        with jax.named_scope("own_on"):
            recv_group(q, 0)
            start_all(both(q, 0, 2))

    def line_out(q):
        with jax.named_scope("line_out"):
            recv_group(q, 1)
            start_all(both(q, 1, 0))
            if isinstance(q, int) and q == FIRST:
                return
            start_all(both(q, 1, 1))

    def line_on(q):
        with jax.named_scope("line_on"):
            recv_group(q, 2)
            start_all(both(q, 1, 2))

    def plane_done(q):
        with jax.named_scope("plane_done"):
            recv_group(q, 3)

    lane = lax.broadcasted_iota(jnp.int32, (ROWS, 128), 1)
    lane_f = lane.astype(F32)

    def spread(index):
        hit = (lane_f == index) | (lane_f == index + 16.0) | (lane_f == index + 32.0)
        return jnp.where(hit, 1.0, 0.0).astype(BF)

    def code(index, q):
        return jnp.dot(
            spread(index), table[:, 1024 * q : 1024 * (q + 1)], preferred_element_type=F32
        )

    def place(k, side, blocks, centre, scale):
        for q in range(2):
            for h in range(2):
                i = 2 * q + h
                values = blocks[i]
                gain = gain_ref[pl.ds(4 * b + i, 1), :]
                xbuf[0, k, i, side] = ((values - centre) * scale * gain).astype(BF)

                @pl.when(mine == i)
                def _(values=values):
                    stream[k, side] = values

    def embed_own(k):
        with jax.named_scope("embed_own"):
            rows = slice(ROWS * k, ROWS * (k + 1))
            p = jnp.broadcast_to(patch_ref[k : k + 1, :], (ROWS, 128)).T[:, 0:1]
            high = (p // 16).astype(F32)
            low = (p % 16).astype(F32)
            slot = lax.broadcasted_iota(jnp.int32, (ROWS, 1), 0) + ROWS * k
            real = jnp.where(slot < counts_ref[0], 1.0, 0.0)
            centre = jnp.zeros((ROWS, 1), F32)
            for q in range(4):
                values = tok[q, rows, :].astype(F32) + code(high if q < 2 else low, q % 2)
                values = jnp.where(real > 0.5, values, 0.0)
                gv[q, 0] = values[:, 0:HALF]
                gv[q, 1] = values[:, HALF:]
                centre = centre + jnp.sum(values, axis=1, keepdims=True)
            centre = centre * (1.0 / D)
            square = jnp.zeros((ROWS, 1), F32)
            for q in range(4):
                for h in range(2):
                    shifted = gv[q, h] - centre
                    square = square + jnp.sum(shifted * shifted, axis=1, keepdims=True)
            scale = lax.rsqrt(square * (1.0 / D) + norm_eps)
            place(k, zh, [gv[2 * b + i // 2, i % 2] for i in range(4)], centre, scale)
            valid[k, zh] = real
            cols = jnp.zeros((ROWS, 128), F32)
            for i, value in enumerate((centre, scale, high, low, real)):
                cols = jnp.where(lane == i, value, cols)
            meta_s[k] = cols.T[0:8, :]

    def meta_copy():
        return remote(meta_s, meta_r, ts_s.at[2], ts_r.at[2], y_peer)

    def share_copy(i):
        ref = oth.at[c, pl.ds(256 * i, 256)]
        return remote(ref, ref, ts_s.at[3 + i], ts_r.at[3 + i], core_peer)

    def embed_other(k):
        with jax.named_scope("embed_other"):
            rows = slice(ROWS * k, ROWS * (k + 1))
            cols = jnp.concatenate([meta_r[k]] * 16, axis=0).T
            centre, scale, high, low, real = [cols[:, i : i + 1] for i in range(5)]
            index = jnp.where(b == 0, high, low)
            blocks = []
            for q in range(2):
                values = oth[q, rows, :].astype(F32) + code(index, q)
                values = jnp.where(real > 0.5, values, 0.0)
                blocks += [values[:, 0:HALF], values[:, HALF:]]
            place(k, 1 - zh, blocks, centre, scale)
            valid[k, 1 - zh] = real

    def share(i):
        with jax.named_scope("token_wait"):
            token_copy(i).wait_recv()
        share_copy(i).start()

    def share(i):
        with jax.named_scope("token_wait"):
            token_copy(i).wait_recv()
        share_copy(i).start()

    def y_copy(k):
        return remote(ysend.at[k], yrecv.at[k], y_s.at[k], y_r.at[k], y_peer)

    def core_copy(s):
        ref = xbuf.at[(s // 4 + 1) % 2, s % 4, mine]
        return remote(ref, ref, xd_s.at[s % 4], xd_r.at[s % 8], core_peer)

    def chip_copy(s):
        ref = xbuf.at[(s // 4 + 1) % 2, s % 4, mine]
        return remote(ref, ref, xi_s.at[s % 4], xi_r.at[s % 8], x_peer)

    def pass_copy(s):
        ref = xbuf.at[(s // 4 + 1) % 2, s % 4, block_of(2)]
        return remote(ref, ref, f_s.at[s % 4], f_r.at[s % 8], core_peer)

    def stat_copies(s):
        return [
            remote(
                statbuf.at[s, 0], statbuf.at[s, r], st_s.at[s % 4], st_r.at[s % 8], column(r)
            )
            for r in range(1, 8)
        ]

    def final_place(k):
        return mixed_out.at[pl.ds(k * ROWS, ROWS), pl.ds(pl.multiple_of(c * HALF, HALF), HALF)]

    def final_copy(k):
        return remote(
            xbuf.at[0, k, 0, a], final_place(k), fin_s.at[0], fin_r.at[0],
            at(x, y, zh, 1 - zl, a),
        )

    def final_core(k):
        return remote(
            xbuf.at[0, k, 0, 1 - a], final_place(k), fin_s.at[1], fin_r.at[0], core_peer
        )

    def normalise(s):
        with jax.named_scope("normalise"):
            last = s - 4
            l, k = s // 4, s % 4
            means = [statbuf[last, r, 0:1, :] for r in range(8)]
            mean = means[0]
            for r in range(1, 8):
                mean = mean + means[r]
            mean = mean * 0.125
            spread_sum = jnp.zeros_like(mean)
            for r in range(8):
                off = means[r] - mean
                spread_sum = spread_sum + (statbuf[last, r, 1:2, :] + float(HALF) * off * off)
            scale = lax.rsqrt(spread_sum * (1.0 / D) + norm_eps)
            rows = jnp.concatenate([means[r] - mean for r in range(4)] + [scale] * 4, axis=0)
            cols = jnp.concatenate([rows] * 16, axis=0).T
            scale = cols[:, 4:5]
            for r in range(4):
                i = block_of(r)
                off = cols[:, r : r + 1]
                gain = gain_ref[pl.ds(8 * l + 4 * b + i, 1), :]
                d = xbuf[l % 2, k, i].reshape(2 * ROWS, HALF).astype(F32)
                xbuf[l % 2, k, i] = ((d + off) * scale * gain).astype(BF).reshape(2, ROWS, HALF)

    def product(s, h, first=0, tiles=2):
        l, k = s // 4, s % 4
        with jax.named_scope("product"):
            left = jnp.concatenate(
                [xbuf[l % 2, k, i].reshape(2 * ROWS, HALF) for i in range(4)], axis=1
            )

            def column_tile(n, _):
                cols = pl.ds(pl.multiple_of(n * 256, 256), 256)
                right = wb[l, h, :, :, :, cols].reshape(2048, 256)
                tile = jnp.dot(left, right, preferred_element_type=F32)
                acc[:, :, cols] = tile.reshape(2, ROWS, 256)
                return 0

            lax.fori_loop(first, first + tiles, column_tile, 0)

    def part_copy(k, i):
        ref = yrecv.at[k, :, :, pl.ds(256 * i, 256)]
        return remote(
            ysend.at[k, :, :, pl.ds(256 * i, 256)], ref, yl_s.at[k, i], yl_r.at[k, i], y_peer
        )

    def give_first(k, i):
        product(k, 1 - b, i, 1)
        cols = slice(256 * i, 256 * (i + 1))
        ysend[k, :, :, cols] = acc[:, :, cols].astype(BF)
        part_copy(k, i).start()

    def received(s):
        k = s % 4

        @pl.when(s < 4)
        def _():
            part_copy(k, 0).wait_recv()
            part_copy(k, 1).wait_recv()

        @pl.when(s >= 4)
        def _():
            y_copy(k).wait_recv()

    def sent_before(s):
        k = s % 4

        @pl.when(s < 8)
        def _():
            part_copy(k, 0).wait_send()
            part_copy(k, 1).wait_send()

        @pl.when(s >= 8)
        def _():
            y_copy(k).wait_send()

    def last_copy(k, i):
        return remote(ysend.at[k, i], yrecv.at[k, i], yl_s.at[k, i], yl_r.at[k, i], y_peer)

    def give(s):
        k = s % 4
        product(s, 1 - b)

        @pl.when(s < STEPS - 4)
        def _():
            ysend[k] = acc[...].astype(BF)
            y_copy(k).start()

        @pl.when(s >= STEPS - 4)
        def _():
            ysend[k, 0] = acc[1 - b].astype(BF)
            last_copy(k, 0).start()
            gv[k, 0] = acc[b]

    def receive(s):
        k = s % 4
        product(s, b)
        with jax.named_scope("y_wait"):
            received(s)
        with jax.named_scope("receive"):
            values = (stream[k] + acc[...] + yrecv[k].astype(F32)).reshape(2 * ROWS, HALF)
            stream[k] = values.reshape(2, ROWS, HALF)
            mean = jnp.sum(values, axis=1, keepdims=True) * (1.0 / HALF)
            d = values - mean
            xbuf[(s // 4 + 1) % 2, k, mine] = d.astype(BF).reshape(2, ROWS, HALF)
            chip_copy(s).start()
            core_copy(s).start()
            square = jnp.sum(d * d, axis=1, keepdims=True)
            lanes = lax.broadcasted_iota(jnp.int32, (2 * ROWS, 128), 1)
            cols = jnp.where(lanes == 0, mean, jnp.where(lanes == 1, square, 0.0))
            statbuf[s, 0] = cols.T[0:2, :]
            start_all(stat_copies(s))

    def give_rest(s):
        k = s % 4
        product(s, b)
        ysend[k, 1] = (acc[1 - b] + stream[k, 1 - b]).astype(BF)
        last_copy(k, 1).start()
        gv[k, 1] = acc[b] + stream[k, b]

    def finish(s, i):
        k = s % 4
        with jax.named_scope("y_wait"):
            last_copy(k, 1 - i).wait_recv()
        with jax.named_scope("finish"):
            real = valid[k, zh] > 0.5
            values = gv[k, i] + yrecv[k, 1 - i].astype(F32)
            xbuf[0, k, 0, i] = jnp.where(real, values, 0.0).astype(BF)

    def finish_both(s):
        k = s % 4
        finish(s, a)
        final_copy(k).start()
        finish(s, 1 - a)

        @pl.when(c == a)
        def _():
            dst = final_place(k)
            pltpu.make_async_copy(xbuf.at[0, k, 0, 1 - a], dst, fin_r.at[0]).start()

        @pl.when(c != a)
        def _():
            final_core(k).start()

    def body(s, _):
        @pl.when((s >= 4) & (s < STEPS))
        def _():
            with jax.named_scope("chip_wait"):
                chip_copy(s - 4).wait_recv()
            pass_copy(s - 4).start()

        @pl.when(s < STEPS - 2)
        def _():
            @pl.when(s % 4 == 2)
            def _():
                plane_done((s - 2) // 2 + 1)

            receive(s - 2)

        @pl.when((s == STEPS - 3) | (s == STEPS - 2))
        def _():
            @pl.when(s == STEPS - 3)
            def _():
                plane_done(2 * LAYERS - 1)

            give_rest(s - 1)

        @pl.when(s >= STEPS - 1)
        def _():
            finish_both(s - 3)

        @pl.when((s >= 4) & (s < STEPS))
        def _():
            last = s - 4
            with jax.named_scope("stat_wait"):
                sent_before(s)
                seven = statbuf.at[last, pl.ds(1, 7)]
                pltpu.make_async_copy(seven, seven, st_s.at[last % 4]).wait()
                pltpu.make_async_copy(seven, seven, st_r.at[last % 8]).wait()
            with jax.named_scope("block_wait"):
                core_copy(last).wait()
                chip_copy(last).wait_send()
                pass_copy(last).wait()
            normalise(s)

            @pl.when(s % 4 == 0)
            def _():
                plane_done(s // 2)

            late = s >= STEPS - 2

            @pl.when(late & (a == 0))
            def _():
                give_rest(s)

            give(s)

            @pl.when(late & (a == 1))
            def _():
                give_rest(s)

        @pl.when((s % 2 == 0) & (s < STEPS - 2))
        def _():
            q = s // 2 + 1

            @pl.when(q + 1 < 2 * LAYERS)
            def _():
                own_on(q + 1)

            line_on(q)

            @pl.when(q + 2 < 2 * LAYERS)
            def _():
                own_out(q + 2)

        @pl.when((s % 2 == 1) & (s < STEPS - 3))
        def _():
            line_out((s + 3) // 2)

        return 0

    weights_kept()
    own_out(0)
    own_out(FIRST)
    embed_own(0)
    own_on(0)
    own_on(FIRST)
    own_out(1)
    embed_own(1)
    line_out(0)
    line_out(FIRST)
    embed_own(2)
    own_on(1)
    embed_own(3)
    meta_copy().start()
    start_outputs()
    line_on(0)
    start_all(both(FIRST, 1, 1))
    share(0)
    with jax.named_scope("meta_wait"):
        meta_copy().wait_recv()
        share_copy(0).wait_recv()
    line_on(FIRST)
    own_out(2)
    embed_other(0)
    weights_sent()
    plane_done(0)
    give_first(0, 0)
    line_out(1)
    share(1)
    embed_other(1)
    give_first(1, 0)
    own_on(2)
    plane_done(FIRST)
    give_first(0, 1)
    give_first(1, 1)
    line_on(1)
    own_out(3)
    with jax.named_scope("share_wait"):
        share_copy(1).wait_recv()
    embed_other(2)
    give_first(2, 0)
    give_first(2, 1)
    embed_other(3)
    line_out(2)
    plane_done(1)
    receive(0)
    give_first(3, 0)
    give_first(3, 1)
    own_on(3)
    line_on(2)
    own_out(4)
    lax.fori_loop(3, STEPS + 3, body, 0)

    with jax.named_scope("final_wait"):
        pltpu.make_async_copy(mixed_out, mixed_out, fin_r.at[0]).wait()
    four_blocks(fin_s.at[0])

    @pl.when(c != a)
    def _():
        four_blocks(fin_s.at[1])

    for k in range(CHUNKS):
        for i in range(2):
            last_copy(k, i).wait_send()
    with jax.named_scope("end_wait"):
        meta_copy().wait_send()
    for i in range(2):
        token_copy(i).wait_send()
        share_copy(i).wait_send()
    blocks = wb.at[0, :, pl.ds(0, 3)]
    for i in range(LAYERS + 1):
        pltpu.make_async_copy(blocks, blocks, ag_s.at[i]).wait()
    for j, dst in enumerate((pv, mv, vv)):
        pltpu.make_async_copy(dst, dst, out_sem.at[j]).wait()


def hand_over(p, m, v, mixed, p_out, m_out, v_out, mixed_out, sem):
    copies = [
        pltpu.make_async_copy(src, dst, sem.at[j])
        for j, (src, dst) in enumerate(((p, p_out), (m, m_out), (v, v_out), (mixed, mixed_out)))
    ]
    for copy in copies:
        copy.start()
    for copy in copies:
        copy.wait()


def per_device(
    tokens, counts, patch_index, clip_limit, norm_gain, params, moments, seconds, gradients
):
    any_space = pl.BlockSpec(memory_space=pl.ANY)
    hbm = pl.BlockSpec(memory_space=pltpu.HBM)
    smem = pl.BlockSpec(memory_space=pltpu.SMEM)
    master = jax.ShapeDtypeStruct((LAYERS, ROWS, 1024), F32)
    dma = pltpu.SemaphoreType.DMA
    shapes = (master, master, master, jax.ShapeDtypeStruct((512, 1024), BF))
    results = pl.pallas_call(
        kernel,
        out_shape=shapes,
        in_specs=[hbm, smem, hbm, smem, hbm] + [hbm] * 4,
        out_specs=(any_space,) * 4,
        scratch_shapes=[
            pltpu.VMEM((LAYERS, ROWS, 1024), F32),
            pltpu.VMEM((LAYERS, ROWS, 1024), F32),
            pltpu.VMEM((LAYERS, ROWS, 1024), F32),
            pltpu.VMEM((LAYERS, 2, ROWS, HALF), F32),
            pltpu.VMEM((LAYERS, 2, 4, 4, ROWS, HALF), BF),
            pltpu.VMEM((4, 512, 1024), BF),
            pltpu.VMEM((2, 512, 1024), BF),
            pltpu.VMEM((2, CHUNKS, 4, 2, ROWS, HALF), BF),
            pltpu.VMEM((CHUNKS, 2, ROWS, HALF), F32),
            pltpu.VMEM((CHUNKS, 2, ROWS, HALF), BF),
            pltpu.VMEM((CHUNKS, 2, ROWS, HALF), BF),
            pltpu.VMEM((2, ROWS, HALF), F32),
            pltpu.VMEM((STEPS - 4, 8, 2, 2 * ROWS), F32),
            pltpu.VMEM((128, 2048), BF),
            pltpu.VMEM((CHUNKS, 2, ROWS, 1), F32),
            pltpu.VMEM((CHUNKS, 8, 128), F32),
            pltpu.VMEM((CHUNKS, 8, 128), F32),
            pltpu.VMEM((2, 16, 8, 128), F32),
            pltpu.VMEM((CHUNKS, 128), jnp.int32),
            pltpu.VMEM((LAYERS, D), F32),
            pltpu.VMEM((32, HALF), F32),
            dma((LAYERS, 2)),
            dma((3,)),
            dma((1,)),
            dma((2,)),
            dma((2,)),
            dma((2,)),
            dma((2,)),
            dma((LAYERS, 2)),
            dma((LAYERS + 1,)),
            dma((2 * LAYERS + 1, 4)),
            dma((5,)),
            dma((5,)),
            dma((4,)),
            dma((4,)),
            dma((CHUNKS, 2)),
            dma((CHUNKS, 2)),
            dma((4,)),
            dma((8,)),
            dma((4,)),
            dma((8,)),
            dma((4,)),
            dma((8,)),
            dma((4,)),
            dma((8,)),
            dma((2,)),
            dma((1,)),
        ],
        compiler_params=pltpu.CompilerParams(
            collective_id=0, has_side_effects=True, vmem_limit_bytes=49200000
        ),
    )(
        tokens,
        counts,
        pltpu.with_memory_space_constraint(patch_index, pltpu.HBM),
        clip_limit.reshape(1, 1),
        pltpu.with_memory_space_constraint(norm_gain, pltpu.HBM),
        params,
        moments,
        seconds,
        gradients,
    )
    return pl.pallas_call(
        hand_over,
        out_shape=shapes,
        in_specs=[any_space] * 4,
        out_specs=(any_space,) * 4,
        scratch_shapes=[
            dma((4,)),
        ],
        compiler_params=pltpu.CompilerParams(vmem_limit_bytes=1024 * 1024),
    )(*results)


def solution(mesh):
    shard = P(None, "dp", "fsdp")
    return jax.shard_map(
        per_device,
        mesh=mesh,
        in_specs=(P("dp", None), P("dp"), P("dp"), P(), P(), shard, shard, shard, shard),
        out_specs=(shard, shard, shard, P("dp", "fsdp")),
        check_vma=False,
    )
```
